8 devices in a mesh: dp: 1 (over z), ei: 2 (over y), eo: 4 (over x, core).
Axes of the slice: x: 2, y: 2, z: 1, core: 2. Of those that a mesh axis runs over, the one named last changes fastest.
Arguments:
- x_tokens: bfloat16 [16384, 1536], P(('dp', 'ei', 'eo'))
- expert_ids: int32 [16384, 6], P(('dp', 'ei', 'eo'))
- gate_vals: float32 [16384, 6], P(('dp', 'ei', 'eo'))
- w_gate: bfloat16 [64, 1536, 512], P(('ei', 'eo'))
- w_up: bfloat16 [64, 1536, 512], P(('ei', 'eo'))
- w_down: bfloat16 [64, 512, 1536], P(('ei', 'eo'))
- ws_gate: bfloat16 [1536, 1024], replicated
- ws_up: bfloat16 [1536, 1024], replicated
- ws_down: bfloat16 [1024, 1536], replicated
- dy_tokens: bfloat16 [16384, 1536], P(('dp', 'ei', 'eo'))
Outputs:
- output 1: bfloat16 [16384, 1536], P(('dp', 'ei', 'eo'))
- output 2: bfloat16 [16384, 1536], P(('dp', 'ei', 'eo'))
- output 3: float32 [16384, 6], P(('dp', 'ei', 'eo'))
- output 4: bfloat16 [64, 1536, 512], P(('dp', 'ei', 'eo'))
- output 5: bfloat16 [64, 1536, 512], P(('dp', 'ei', 'eo'))
- output 6: bfloat16 [64, 512, 1536], P(('dp', 'ei', 'eo'))
- output 7: float32 [1536, 1024], P('dp')
- output 8: float32 [1536, 1024], P('dp')
- output 9: float32 [1024, 1536], P('dp')
All inputs are finite; a program needn't handle non-finite values.
Results may differ from the reference program's by a relative error of at most 0.00113.
Values are sent between devices in bfloat16 or wider.
A program may use at most 1 GiB of HBM per device.

```python
import jax
import jax.numpy as jnp
from jax import lax

D = 1536
F = 512
FS = 1024
EXPERTS = 64
TOP = 6
TOK = 2048
EI = 2
EO = 4
CAP_FACTOR = 2

GROUP = EI * EO
ROWS = GROUP * TOK
CAP = min(TOK, CAP_FACTOR * ((TOK * TOP + EXPERTS - 1) // EXPERTS))
HOT = EXPERTS // 4


def route_one(dev_key):
    perm_key, tok_key, rot_key = jax.random.split(dev_key, 3)
    total_count = TOK * TOP
    cold_total = total_count - HOT * CAP
    cold_experts = EXPERTS - HOT
    base_count = cold_total // cold_experts
    extra_count = cold_total % cold_experts
    positions = jnp.arange(EXPERTS, dtype=jnp.int32)
    counts = jnp.where(positions < HOT, CAP, base_count + (positions - HOT < extra_count).astype(jnp.int32))
    run_ends = jnp.cumsum(counts)
    run_pos = jnp.searchsorted(run_ends, jnp.arange(total_count, dtype=jnp.int32), side='right')
    labels = jax.random.permutation(perm_key, EXPERTS)
    id_table = labels[run_pos].reshape(TOP, TOK).T
    id_table = id_table[jax.random.permutation(tok_key, TOK)]
    col_shift = jax.random.randint(rot_key, (TOK, 1), 0, TOP)
    col_order = (jnp.arange(TOP)[None, :] + col_shift) % TOP
    return jnp.take_along_axis(id_table, col_order, axis=1).astype(jnp.int32)


def draw_routing(route_key):
    dev_keys = jax.random.split(route_key, GROUP)
    return jax.vmap(route_one)(dev_keys).reshape(ROWS, TOP)


def setup_inputs(seed: int = 0, part: int = 0) -> dict:
    root_key = jax.random.key(seed)
    shared_key, part_root = jax.random.split(root_key)
    part_key = jax.random.fold_in(part_root, part)
    key_list = jax.random.split(part_key, 4)
    weight_keys = jax.random.split(shared_key, 6)
    x_tokens = jax.random.normal(key_list[0], (ROWS, D), jnp.float32).astype(jnp.bfloat16)
    expert_ids = draw_routing(key_list[1])
    gate_vals = jax.random.uniform(key_list[2], (ROWS, TOP), jnp.float32, 0.05, 0.3)
    dy_tokens = jax.random.normal(key_list[3], (ROWS, D), jnp.float32).astype(jnp.bfloat16)
    w_gate = (jax.random.normal(weight_keys[0], (EXPERTS, D, F), jnp.float32) * D ** -0.5).astype(jnp.bfloat16)
    w_up = (jax.random.normal(weight_keys[1], (EXPERTS, D, F), jnp.float32) * D ** -0.5).astype(jnp.bfloat16)
    w_down = (jax.random.normal(weight_keys[2], (EXPERTS, F, D), jnp.float32) * F ** -0.5).astype(jnp.bfloat16)
    ws_gate = (jax.random.normal(weight_keys[3], (D, FS), jnp.float32) * D ** -0.5).astype(jnp.bfloat16)
    ws_up = (jax.random.normal(weight_keys[4], (D, FS), jnp.float32) * D ** -0.5).astype(jnp.bfloat16)
    ws_down = (jax.random.normal(weight_keys[5], (FS, D), jnp.float32) * FS ** -0.5).astype(jnp.bfloat16)
    return {'x_tokens': x_tokens, 'expert_ids': expert_ids, 'gate_vals': gate_vals, 'w_gate': w_gate, 'w_up': w_up, 'w_down': w_down, 'ws_gate': ws_gate, 'ws_up': ws_up, 'ws_down': ws_down, 'dy_tokens': dy_tokens}


def silu_grad(pre_act):
    sigmoid_val = jax.nn.sigmoid(pre_act)
    return sigmoid_val * (1.0 + pre_act * (1.0 - sigmoid_val))


def reference(x_tokens, expert_ids, gate_vals, w_gate, w_up, w_down, ws_gate, ws_up, ws_down, dy_tokens):
    flat_ids = expert_ids.reshape(-1)
    flat_gates = gate_vals.reshape(-1)
    order_ids = jnp.argsort(flat_ids, stable=True)
    counts = jnp.bincount(flat_ids, length=EXPERTS)
    starts = jnp.cumsum(counts) - counts
    max_rows = GROUP * CAP
    padded = jnp.concatenate([order_ids, jnp.zeros((max_rows,), order_ids.dtype)])
    row_index = jnp.arange(max_rows)

    def expert_step(carry_in, per_expert):
        y_acc, dx_acc, dg_acc = carry_in
        w_one, w_three, w_two, start_at, count_at = per_expert
        slot_ids = lax.dynamic_slice(padded, (start_at,), (max_rows,))
        valid_row = row_index < count_at
        tok_ids = slot_ids // TOP
        x_rows = jnp.where(valid_row[:, None], x_tokens[tok_ids], 0)
        pre_one = jnp.dot(x_rows, w_one, preferred_element_type=jnp.float32)
        pre_three = jnp.dot(x_rows, w_three, preferred_element_type=jnp.float32)
        act_h = (jax.nn.silu(pre_one) * pre_three).astype(jnp.bfloat16)
        out_rows = jnp.dot(act_h, w_two, preferred_element_type=jnp.float32).astype(jnp.bfloat16)
        gate_rows = jnp.where(valid_row, flat_gates[slot_ids], 0.0)
        dy_rows = dy_tokens[tok_ids].astype(jnp.float32)
        do_rows = (gate_rows[:, None] * dy_rows).astype(jnp.bfloat16)
        y_acc = y_acc.at[tok_ids].add(gate_rows[:, None] * out_rows.astype(jnp.float32))
        dg_rows = jnp.where(valid_row, jnp.sum(dy_rows * out_rows.astype(jnp.float32), axis=1), 0.0)
        dg_acc = dg_acc.at[slot_ids].add(dg_rows)
        grad_h = jnp.dot(do_rows, w_two.T, preferred_element_type=jnp.float32)
        da_one = (grad_h * pre_three * silu_grad(pre_one)).astype(jnp.bfloat16)
        da_three = (grad_h * jax.nn.silu(pre_one)).astype(jnp.bfloat16)
        dx_rows = (jnp.dot(da_one, w_one.T, preferred_element_type=jnp.float32) + jnp.dot(da_three, w_three.T, preferred_element_type=jnp.float32)).astype(jnp.bfloat16)
        dx_acc = dx_acc.at[tok_ids].add(dx_rows.astype(jnp.float32))
        dw_one = jnp.dot(x_rows.T, da_one, preferred_element_type=jnp.float32).astype(jnp.bfloat16)
        dw_three = jnp.dot(x_rows.T, da_three, preferred_element_type=jnp.float32).astype(jnp.bfloat16)
        dw_two = jnp.dot(act_h.T, do_rows, preferred_element_type=jnp.float32).astype(jnp.bfloat16)
        return (y_acc, dx_acc, dg_acc), (dw_one, dw_three, dw_two)

    carry_init = (jnp.zeros((ROWS, D), jnp.float32), jnp.zeros((ROWS, D), jnp.float32), jnp.zeros((ROWS * TOP,), jnp.float32))
    carry_out, weight_grads = lax.scan(expert_step, carry_init, (w_gate, w_up, w_down, starts, counts))
    y_acc, dx_acc, dg_acc = carry_out
    dw_gate, dw_up, dw_down = weight_grads
    sh_one = jnp.dot(x_tokens, ws_gate, preferred_element_type=jnp.float32)
    sh_three = jnp.dot(x_tokens, ws_up, preferred_element_type=jnp.float32)
    sh_act = (jax.nn.silu(sh_one) * sh_three).astype(jnp.bfloat16)
    y_tokens = (y_acc + jnp.dot(sh_act, ws_down, preferred_element_type=jnp.float32)).astype(jnp.bfloat16)
    grad_sh = jnp.dot(dy_tokens, ws_down.T, preferred_element_type=jnp.float32)
    ds_one = (grad_sh * sh_three * silu_grad(sh_one)).astype(jnp.bfloat16)
    ds_three = (grad_sh * jax.nn.silu(sh_one)).astype(jnp.bfloat16)
    dx_shared = jnp.dot(ds_one, ws_gate.T, preferred_element_type=jnp.float32) + jnp.dot(ds_three, ws_up.T, preferred_element_type=jnp.float32)
    dx_tokens = (dx_acc + dx_shared).astype(jnp.bfloat16)
    dws_gate = jnp.dot(x_tokens.T, ds_one, preferred_element_type=jnp.float32)
    dws_up = jnp.dot(x_tokens.T, ds_three, preferred_element_type=jnp.float32)
    dws_down = jnp.dot(sh_act.T, dy_tokens, preferred_element_type=jnp.float32)
    d_gates = dg_acc.reshape(ROWS, TOP)
    return (y_tokens, dx_tokens, d_gates, dw_gate, dw_up, dw_down, dws_gate, dws_up, dws_down)
```

```python
import functools

import jax
import jax.numpy as jnp
from jax import lax
from jax.experimental import pallas as pl
from jax.experimental.pallas import tpu as pltpu
from jax.sharding import PartitionSpec as P

CAP_FACTOR = 2
CHUNKS = 4
BLK = 256
LANE = 128
SUB = 8
STAGE = 512
F32 = jnp.float32
BF16 = jnp.bfloat16


def silu_grad(pre_act):
    sigmoid_val = jax.nn.sigmoid(pre_act)
    return sigmoid_val * (1.0 + pre_act * (1.0 - sigmoid_val))


SMEM = pl.BlockSpec(memory_space=pltpu.SMEM)
HBM = pl.BlockSpec(memory_space=pl.ANY)
PARAMS = dict(vmem_limit_bytes=60 << 20)


def pipeline(body, n, in_specs=(), out_specs=()):
    return pltpu.emit_pipeline(lambda at, *refs: body(at.index[0], *refs), grid=(n,), in_specs=in_specs, out_specs=out_specs, _explicit_indices=True)


def gather_kernel(chunk_tok, dim, slot_cap, blk_e, blk_k, meta, slots, gsel, tok_hbm, *refs):
    x_out, dy_out, g_out, stage, rowbuf = refs[-5:]
    n_groups = dim // LANE
    off = meta[1]
    stage[chunk_tok // SUB] = jnp.zeros(stage.shape[1:], F32)

    def fill(step, tok_ref):
        def convert(i, carry):
            for c in range(n_groups):
                val = tok_ref[pl.ds(pl.multiple_of(i * 16, 16), 16), c * LANE:(c + 1) * LANE].astype(F32)
                at = step * (STAGE // SUB) + 2 * i
                stage[at, c * SUB:(c + 1) * SUB, :] = val[:SUB]
                stage[at + 1, c * SUB:(c + 1) * SUB, :] = val[SUB:]
            return carry
        lax.fori_loop(0, STAGE // 16, convert, 0)

    def rows(b, rows_ref, *gate):
        e = blk_e[b]
        base = e * slot_cap + blk_k[b] * BLK

        def move(g, carry):
            vals = []
            for r in range(SUB):
                t = slots[base + g * SUB + r]
                hi = t >> 3
                lo = t & 7
                vals.append((stage[hi, pl.ds(lo, 8, stride=SUB), :], stage[hi, pl.ds(lo + 64, n_groups - 8, stride=SUB), :]))
                if gate:
                    gate[0][g, r:r + 1, :] = jnp.full((1, LANE), gsel[e * chunk_tok + t], F32)
            for r in range(SUB):
                rowbuf[g, pl.ds(r, 8, stride=SUB), :] = vals[r][0]
                rowbuf[g, pl.ds(r + 64, n_groups - 8, stride=SUB), :] = vals[r][1]
            return carry
        lax.fori_loop(0, BLK // SUB, move, 0)

        def pack(i, carry):
            for c in range(n_groups):
                a = rowbuf[2 * i, c * SUB:(c + 1) * SUB, :]
                b2 = rowbuf[2 * i + 1, c * SUB:(c + 1) * SUB, :]
                rows_ref[pl.ds(pl.multiple_of(i * 16, 16), 16), c * LANE:(c + 1) * LANE] = jnp.concatenate([a, b2], axis=0).astype(BF16)
            return carry
        lax.fori_loop(0, BLK // 16, pack, 0)

    row_spec = pl.BlockSpec((BLK, dim), lambda i: (off + i, 0))
    gate_spec = pl.BlockSpec((BLK // SUB, SUB, LANE), lambda i: (off + i, 0, 0))
    n_stage = chunk_tok // STAGE
    pipeline(fill, n_stage, in_specs=[pl.BlockSpec((STAGE, dim), lambda i: (2 * i, 0))])(tok_hbm)
    pipeline(rows, meta[0], out_specs=[row_spec])(x_out)
    pipeline(fill, n_stage, in_specs=[pl.BlockSpec((STAGE, dim), lambda i: (2 * i + 1, 0))])(tok_hbm)
    pipeline(rows, meta[0], out_specs=[row_spec, gate_spec])(dy_out, g_out)


def gather_rows(tok, held, tables, n_rows):
    chunk_tok, dim = tok.shape[0] // 2, tok.shape[1]
    slot_cap = tables[3].shape[0] // 8
    return pl.pallas_call(
        functools.partial(gather_kernel, chunk_tok, dim, slot_cap),
        out_shape=[jax.ShapeDtypeStruct((n_rows, dim), BF16), jax.ShapeDtypeStruct((n_rows, dim), BF16),
                   jax.ShapeDtypeStruct((n_rows // SUB, SUB, LANE), F32)],
        in_specs=[SMEM] * 5 + [HBM] * (1 + len(held)),
        out_specs=[HBM] * 3,
        scratch_shapes=[pltpu.VMEM((chunk_tok // SUB + 1, dim // LANE * SUB, LANE), F32),
                        pltpu.VMEM((BLK // SUB, dim // LANE * SUB, LANE), F32)],
        input_output_aliases={6 + i: i for i in range(len(held))},
        compiler_params=pltpu.CompilerParams(**PARAMS),
        cost_estimate=pl.CostEstimate(flops=60_000_000_000, bytes_accessed=120_000_000, transcendentals=0),
        name="gather_rows",
    )(*tables, tok, *held)


def scale_rows(gate, dy):
    return jnp.concatenate([(gate * dy[:, c * LANE:(c + 1) * LANE]).astype(BF16) for c in range(dy.shape[1] // LANE)], axis=1)


def expert_body(e, x_ref, dy_ref, g_ref, w1_ref, w3_ref, w2_ref, o_ref, dx_ref, dg_ref, h_ref, d1_ref, d3_ref):
    x = x_ref[...]
    dot = functools.partial(jnp.dot, preferred_element_type=F32)
    dot_t = lambda a, b: lax.dot_general(a, b, (((1,), (1,)), ((), ())), preferred_element_type=F32)
    a1 = dot(x, w1_ref[0])
    a3 = dot(x, w3_ref[0])
    sig = jax.nn.sigmoid(a1)
    act = a1 * sig
    h = (act * a3).astype(BF16)
    h_ref[...] = h
    o = dot(h, w2_ref[0]).astype(BF16)
    o_ref[...] = o
    dy = dy_ref[...].astype(F32)
    prod = dy * o.astype(F32)
    part = prod[:, 0:LANE]
    for c in range(1, prod.shape[1] // LANE):
        part = part + prod[:, c * LANE:(c + 1) * LANE]
    dg = jnp.sum(part, axis=1, keepdims=True)
    lane = lax.broadcasted_iota(jnp.int32, part.shape, 1)
    dg_ref[...] = jnp.where(lane == e, dg, 0.0)
    dh = dot_t(scale_rows(g_ref[...], dy), w2_ref[0])
    d1 = (dh * a3 * (sig * (1.0 + a1 * (1.0 - sig)))).astype(BF16)
    d3 = (dh * act).astype(BF16)
    d1_ref[...] = d1
    d3_ref[...] = d3
    dx_ref[...] = (dot_t(d1, w1_ref[0]) + dot_t(d3, w3_ref[0])).astype(BF16)


def expert_kernel(blk_e, meta, x, dy, g, w1, w3, w2, *refs):
    outs = refs[-6:]
    dim, ffn = w1.shape[1:]
    off = meta[1]
    glob = lambda i: (off + i, 0)
    loc = lambda i: (i, 0)
    wmap = lambda i: (blk_e[i], 0, 0)
    pipeline(
        lambda b, *refs: expert_body(blk_e[b], *refs), meta[0],
        in_specs=[pl.BlockSpec((BLK, dim), glob), pl.BlockSpec((BLK, dim), glob), pl.BlockSpec((BLK, LANE), glob),
                  pl.BlockSpec((1, dim, ffn), wmap), pl.BlockSpec((1, dim, ffn), wmap), pl.BlockSpec((1, ffn, dim), wmap)],
        out_specs=[pl.BlockSpec((BLK, dim), loc), pl.BlockSpec((BLK, dim), loc), pl.BlockSpec((BLK, LANE), loc)]
        + [pl.BlockSpec((BLK, ffn), glob)] * 3)(x, dy, g, w1, w3, w2, *outs)


def run_experts(x_rows, dy_rows, gates, w1, w3, w2, saved, blk_e, meta):
    n_rows, dim = x_rows.shape
    loc_rows = blk_e.shape[0] * BLK
    return pl.pallas_call(
        expert_kernel,
        out_shape=[jax.ShapeDtypeStruct((loc_rows, dim), BF16), jax.ShapeDtypeStruct((loc_rows, dim), BF16),
                   jax.ShapeDtypeStruct((loc_rows, LANE), F32)] + [jax.ShapeDtypeStruct((n_rows, w1.shape[2]), BF16)] * 3,
        in_specs=[SMEM] * 2 + [HBM] * (6 + len(saved)),
        out_specs=[HBM] * 6,
        input_output_aliases={8 + i: 3 + i for i in range(len(saved))},
        compiler_params=pltpu.CompilerParams(**PARAMS),
        cost_estimate=pl.CostEstimate(flops=60_000_000_000, bytes_accessed=80_000_000, transcendentals=0),
        name="experts",
    )(blk_e, meta, x_rows, dy_rows, gates, w1, w3, w2, *saved)


def combine_kernel(n_groups, slot_cap, blk_e, blk_k, meta, slots, o_hbm, g_hbm, dg_hbm, dx_hbm, out_ref, dgo_ref, stage_y, stage_dx, rowbuf, sem):
    n_tiles = out_ref.shape[0]
    dim = n_groups * LANE
    used = n_groups * SUB
    off = meta[1]

    def rows(stage, planes, b, rows_ref, *gate):
        base = blk_e[b] * slot_cap + blk_k[b] * BLK

        def unpack(i, carry):
            if gate:
                ga = gate[0][2 * i]
                gb = gate[0][2 * i + 1]
            for c in range(n_groups):
                val = rows_ref[pl.ds(pl.multiple_of(i * 16, 16), 16), c * LANE:(c + 1) * LANE].astype(F32)
                lo, hi = val[:SUB], val[SUB:]
                if gate:
                    lo, hi = lo * ga, hi * gb
                rowbuf[2 * i, c * SUB:(c + 1) * SUB, :] = lo
                rowbuf[2 * i + 1, c * SUB:(c + 1) * SUB, :] = hi
            if gate:
                rowbuf[2 * i, used:, :] = gate[1][2 * i]
                rowbuf[2 * i + 1, used:, :] = gate[1][2 * i + 1]
            return carry
        lax.fori_loop(0, BLK // 16, unpack, 0)

        def add(g, carry):
            todo = []
            for r in range(SUB):
                t = slots[base + g * SUB + r]
                hi = t >> 3
                lo = t & 7
                a = stage[hi, pl.ds(lo, 8, stride=SUB), :] + rowbuf[g, pl.ds(r, 8, stride=SUB), :]
                c = stage[hi, pl.ds(lo + 64, planes - 8, stride=SUB), :] + rowbuf[g, pl.ds(r + 64, planes - 8, stride=SUB), :]
                todo.append((hi, lo, a, c))
            for hi, lo, a, c in todo:
                stage[hi, pl.ds(lo, 8, stride=SUB), :] = a
                stage[hi, pl.ds(lo + 64, planes - 8, stride=SUB), :] = c
            return carry
        lax.fori_loop(0, BLK // SUB, add, 0)

    def clear(stage):
        def zero(i, carry):
            stage[i] = jnp.zeros(stage.shape[1:], F32)
            return carry
        lax.fori_loop(0, n_tiles + 1, zero, 0)

    row_spec = pl.BlockSpec((BLK, dim), lambda i: (i, 0))
    gate_spec = pl.BlockSpec((BLK // SUB, SUB, LANE), lambda i: (off + i, 0, 0))
    dg_spec = pl.BlockSpec((BLK // SUB, SUB, LANE), lambda i: (i, 0, 0))
    tiles = pl.ds(0, n_tiles)
    copies = [pltpu.make_async_copy(stage_y.at[tiles, pl.ds(0, used)], out_ref.at[:, pl.ds(0, used)], sem.at[0]),
              pltpu.make_async_copy(stage_y.at[tiles, pl.ds(used, SUB)], dgo_ref, sem.at[1]),
              pltpu.make_async_copy(stage_dx.at[tiles], out_ref.at[:, pl.ds(used, used)], sem.at[2])]
    clear(stage_y)
    pipeline(functools.partial(rows, stage_y, n_groups + 1), meta[0], in_specs=[row_spec, gate_spec, dg_spec])(o_hbm, g_hbm, dg_hbm)
    copies[0].start()
    copies[1].start()
    clear(stage_dx)
    pipeline(functools.partial(rows, stage_dx, n_groups), meta[0], in_specs=[row_spec])(dx_hbm)
    copies[2].start()
    for copy in copies:
        copy.wait()


def combine_rows(o_rows, gates, dg, dx_rows, tables, chunk_tok):
    n_groups = o_rows.shape[1] // LANE
    slot_cap = tables[3].shape[0] // 8
    n_tiles = chunk_tok // SUB
    return pl.pallas_call(
        functools.partial(combine_kernel, n_groups, slot_cap),
        out_shape=[jax.ShapeDtypeStruct((n_tiles, 2 * n_groups * SUB, LANE), F32), jax.ShapeDtypeStruct((n_tiles, SUB, LANE), F32)],
        in_specs=[SMEM] * 4 + [HBM] * 4,
        out_specs=[HBM] * 2,
        scratch_shapes=[pltpu.VMEM((n_tiles + 1, (n_groups + 1) * SUB, LANE), F32), pltpu.VMEM((n_tiles + 1, n_groups * SUB, LANE), F32),
                        pltpu.VMEM((BLK // SUB, (n_groups + 1) * SUB, LANE), F32), pltpu.SemaphoreType.DMA((3,))],
        compiler_params=pltpu.CompilerParams(**PARAMS),
        cost_estimate=pl.CostEstimate(flops=80_000_000_000, bytes_accessed=120_000_000, transcendentals=0),
        name="combine_rows",
    )(*tables[:4], o_rows, gates, dg, dx_rows)


def grad_kernel(order, owner, total, x, dy, g, h, d1, d3, o1, o3, o2, acc1, acc3, acc2):
    dim, ffn = o1.shape[1:]
    n = total[0]

    def step(i, x_ref, dy_ref, g_ref, h_ref, d1_ref, d3_ref, o1_ref, o3_ref, o2_ref):
        e = owner[i]
        first = jnp.logical_or(i == 0, owner[jnp.maximum(i - 1, 0)] != e)
        last = jnp.logical_or(i == n - 1, owner[jnp.minimum(i + 1, owner.shape[0] - 1)] != e)

        @pl.when(first)
        def _():
            acc1[...] = jnp.zeros_like(acc1)
            acc3[...] = jnp.zeros_like(acc3)
            acc2[...] = jnp.zeros_like(acc2)

        dot_l = lambda a, b: lax.dot_general(a, b, (((0,), (0,)), ((), ())), preferred_element_type=F32)
        x = x_ref[...]
        acc1[...] += dot_l(x, d1_ref[...])
        acc3[...] += dot_l(x, d3_ref[...])
        acc2[...] += dot_l(h_ref[...], scale_rows(g_ref[...], dy_ref[...].astype(F32)))

        @pl.when(last)
        def _():
            o1_ref[0] = acc1[...].astype(BF16)
            o3_ref[0] = acc3[...].astype(BF16)
            o2_ref[0] = acc2[...].astype(BF16)
    row = lambda i: (order[i], 0)
    wmap = lambda i: (owner[i], 0, 0)
    pipeline(
        step, n,
        in_specs=[pl.BlockSpec((BLK, dim), row), pl.BlockSpec((BLK, dim), row), pl.BlockSpec((BLK, LANE), row)]
        + [pl.BlockSpec((BLK, ffn), row)] * 3,
        out_specs=[pl.BlockSpec((1, dim, ffn), wmap), pl.BlockSpec((1, dim, ffn), wmap), pl.BlockSpec((1, ffn, dim), wmap)],
    )(x, dy, g, h, d1, d3, o1, o3, o2)


def weight_grads(x_rows, dy_rows, gates, saved, order, owner, total, n_local):
    dim = x_rows.shape[1]
    ffn = saved[0].shape[1]
    return pl.pallas_call(
        grad_kernel,
        out_shape=[jax.ShapeDtypeStruct((n_local, dim, ffn), BF16), jax.ShapeDtypeStruct((n_local, dim, ffn), BF16),
                   jax.ShapeDtypeStruct((n_local, ffn, dim), BF16)],
        in_specs=[SMEM] * 3 + [HBM] * 6,
        out_specs=[HBM] * 3,
        scratch_shapes=[pltpu.VMEM((dim, ffn), F32), pltpu.VMEM((dim, ffn), F32), pltpu.VMEM((ffn, dim), F32)],
        compiler_params=pltpu.CompilerParams(**PARAMS),
        cost_estimate=pl.CostEstimate(flops=100_000_000_000, bytes_accessed=160_000_000, transcendentals=0),
        name="weight_grads",
    )(order, owner, total, x_rows, dy_rows, gates, *saved)


def route(ids_all, gates_all, first_expert, n_local, slot_cap):
    n_chunk, n_top, chunk_tok = ids_all.shape
    experts = first_expert + jnp.arange(n_local, dtype=jnp.int32)
    match = ids_all[:, None] == experts[None, :, None, None]
    hit = jnp.any(match, axis=2)
    gsel = jnp.sum(jnp.where(match, gates_all[:, None], 0.0), axis=2)
    n_seg = chunk_tok // LANE
    strict = (jnp.arange(LANE)[:, None] < jnp.arange(LANE)[None, :]).astype(BF16)
    seg = hit.reshape(n_chunk, n_local, n_seg, LANE)
    inner = jnp.einsum('cesl,lm->cesm', seg.astype(BF16), strict, preferred_element_type=F32)
    seg_sum = jnp.sum(seg, axis=3, dtype=jnp.int32)
    before = jnp.arange(n_seg)[:, None] < jnp.arange(n_seg)[None, :]
    outer = jnp.sum(jnp.where(before, seg_sum[..., :, None], 0), axis=2)
    rank = (inner.astype(jnp.int32) + outer[..., None]).reshape(n_chunk, n_local, chunk_tok)
    count = jnp.sum(seg_sum, axis=2)
    n_hi = slot_cap // 64
    hi = jnp.where(hit, rank >> 6, -1)
    lo = rank & 63
    pick_hi = (hi[:, :, None, :] == jnp.arange(n_hi, dtype=jnp.int32)[:, None]).astype(BF16)
    tok = jnp.arange(chunk_tok, dtype=jnp.int32)
    pick_lo = lo[:, :, None, :] == jnp.arange(64, dtype=jnp.int32)[:, None]
    val_lo = jnp.concatenate([jnp.where(pick_lo, (tok >> 6), 0), jnp.where(pick_lo, (tok & 63), 0)], axis=2).astype(BF16)
    found = jnp.einsum('ceht,cent->cehn', pick_hi, val_lo, preferred_element_type=F32).astype(jnp.int32)
    slots = (found[..., :64] * 64 + found[..., 64:]).reshape(n_chunk, n_local, slot_cap)
    slots = jnp.where(jnp.arange(slot_cap, dtype=jnp.int32) < count[..., None], slots, chunk_tok)
    n_blk = (count + BLK - 1) // BLK
    upto = jnp.cumsum(n_blk, axis=1)
    chunk_blk = upto[:, -1]
    chunk_off = jnp.cumsum(chunk_blk) - chunk_blk
    max_blk = n_local * (slot_cap // BLK)
    at = jnp.arange(max_blk, dtype=jnp.int32)
    blk_e = jnp.minimum(jnp.sum(at[None, :, None] >= upto[:, None, :], axis=2, dtype=jnp.int32), n_local - 1)
    start = upto - n_blk
    blk_k = at[None, :] - jnp.sum(jnp.where(blk_e[..., None] == jnp.arange(n_local), start[:, None, :], 0), axis=2)
    glob = (chunk_off[:, None] + start).T.reshape(-1)
    cnt = n_blk.T.reshape(-1)
    end = jnp.cumsum(cnt)
    total_blk = end[-1]
    at2 = jnp.arange(n_local * slot_cap // BLK + n_chunk * n_local, dtype=jnp.int32)
    grp = jnp.minimum(jnp.sum(at2[:, None] >= end[None, :], axis=1, dtype=jnp.int32), cnt.shape[0] - 1)
    sel = grp[:, None] == jnp.arange(cnt.shape[0])
    order = at2 + jnp.sum(jnp.where(sel, (glob - (end - cnt))[None, :], 0), axis=1)
    order = jnp.clip(order, 0, at2.shape[0] - 1).astype(jnp.int32)
    owner = (grp // n_chunk).astype(jnp.int32)
    return slots, gsel, blk_e, blk_k.astype(jnp.int32), chunk_blk, chunk_off, order, owner, total_blk


def solution(mesh):
    ei_size = mesh.shape['ei']
    eo_size = mesh.shape['eo']
    group_size = ei_size * eo_size
    axes = ('ei', 'eo')
    tok_spec = P(('dp', 'ei', 'eo'), None)
    exp_spec = P(('ei', 'eo'), None, None)
    full_spec = P(None, None)
    grad_spec = P(('dp', 'ei', 'eo'), None, None)
    shared_spec = P('dp', None)

    def device_step(x_loc, ids_loc, gates_loc, w_one, w_three, w_two, s_one, s_three, s_two, dy_loc):
        n_tok, n_top = ids_loc.shape
        dim = x_loc.shape[1]
        ffn = w_one.shape[2]
        n_local = w_one.shape[0]
        n_exp = n_local * group_size
        cap = min(n_tok, CAP_FACTOR * ((n_tok * n_top + n_exp - 1) // n_exp))
        slot_cap = cap * group_size
        part = n_tok // CHUNKS
        chunk_tok = part * group_size
        me = lax.axis_index('ei') * eo_size + lax.axis_index('eo')

        ids_t = lax.all_gather(ids_loc.T, axes, axis=0)
        gates_t = lax.all_gather(gates_loc.T, axes, axis=0)
        split = lambda v: v.reshape(group_size, n_top, CHUNKS, part).transpose(2, 1, 0, 3).reshape(CHUNKS, n_top, chunk_tok)
        tok_chunks = [lax.all_gather(jnp.concatenate([v[c * part:(c + 1) * part] for v in (x_loc, dy_loc)]), axes, axis=0, tiled=True) for c in range(CHUNKS)]
        slots, gsel, blk_e, blk_k, chunk_blk, chunk_off, order, owner, total_blk = route(
            split(ids_t), split(gates_t), me * n_local, n_local, slot_cap)
        n_rows = order.shape[0] * BLK

        sh_one = jnp.dot(x_loc, s_one, preferred_element_type=F32)
        sh_three = jnp.dot(x_loc, s_three, preferred_element_type=F32)
        sh_act = (jax.nn.silu(sh_one) * sh_three).astype(BF16)
        y_shared = jnp.dot(sh_act, s_two, preferred_element_type=F32)
        grad_sh = jnp.einsum('td,fd->tf', dy_loc, s_two, preferred_element_type=F32)
        ds_one = (grad_sh * sh_three * silu_grad(sh_one)).astype(BF16)
        ds_three = (grad_sh * jax.nn.silu(sh_one)).astype(BF16)
        dx_shared = jnp.einsum('tf,df->td', ds_one, s_one, preferred_element_type=F32) + jnp.einsum('tf,df->td', ds_three, s_three, preferred_element_type=F32)
        dws_one = jnp.einsum('td,tf->df', x_loc, ds_one, preferred_element_type=F32)
        dws_three = jnp.einsum('td,tf->df', x_loc, ds_three, preferred_element_type=F32)
        dws_two = jnp.einsum('tf,td->fd', sh_act, dy_loc, preferred_element_type=F32)

        held, saved = [], []
        sums, dg_parts = [], []
        for c in range(CHUNKS):
            meta = jnp.stack([chunk_blk[c], chunk_off[c]]).astype(jnp.int32)
            gpad = jnp.concatenate([gsel[c].reshape(-1), jnp.zeros((LANE,), F32)])
            tables = (blk_e[c], blk_k[c], meta, slots[c].reshape(-1), gpad)
            x_rows, dy_rows, gate_rows = gather_rows(tok_chunks[c], held, tables, n_rows)
            o_rows, dx_rows, dg, *saved = run_experts(x_rows, dy_rows, gate_rows.reshape(n_rows, LANE), w_one, w_three, w_two, saved, blk_e[c], meta)
            part_sum, dg_part = combine_rows(o_rows, gate_rows, dg.reshape(-1, SUB, LANE), dx_rows, tables, chunk_tok)
            x_rows, part_sum = lax.optimization_barrier((x_rows, part_sum))
            held = [x_rows, dy_rows, gate_rows]
            sums.append(lax.psum_scatter(part_sum, axes, scatter_dimension=0, tiled=True))
            dg_parts.append(dg_part.reshape(group_size, part, LANE)[:, :, :n_local])
        dw_one, dw_three, dw_two = weight_grads(x_rows, dy_rows, gate_rows.reshape(n_rows, LANE), saved, order, owner, total_blk[None], n_local)

        n_groups = dim // LANE
        natural = lambda v: v.reshape(part // SUB, n_groups, SUB, LANE).transpose(0, 2, 1, 3).reshape(part, dim)
        y_loc = (jnp.concatenate([natural(v[:, :n_groups * SUB]) for v in sums]) + y_shared).astype(BF16)
        dx_loc = (jnp.concatenate([natural(v[:, n_groups * SUB:]) for v in sums]) + dx_shared).astype(BF16)
        dg_send = jnp.stack(dg_parts, axis=1)
        dg_recv = lax.all_to_all(dg_send, axes, 0, 0)
        dg_tok = dg_recv.transpose(1, 2, 0, 3).reshape(n_tok, n_exp)
        pick = ids_loc[:, :, None] == jnp.arange(n_exp, dtype=jnp.int32)
        d_gates = jnp.sum(jnp.where(pick, dg_tok[:, None, :], 0.0), axis=2)
        dws_one, dws_three, dws_two = lax.psum((dws_one, dws_three, dws_two), axes)
        return (y_loc, dx_loc, d_gates, dw_one, dw_three, dw_two, dws_one, dws_three, dws_two)

    return jax.shard_map(device_step, mesh=mesh, in_specs=(tok_spec, tok_spec, tok_spec, exp_spec, exp_spec, exp_spec, full_spec, full_spec, full_spec, tok_spec), out_specs=(tok_spec, tok_spec, tok_spec, grad_spec, grad_spec, grad_spec, shared_spec, shared_spec, shared_spec), check_vma=False)
```

```python
import functools

import jax
import jax.numpy as jnp
from jax import lax
from jax.experimental import pallas as pl
from jax.experimental.pallas import tpu as pltpu
from jax.sharding import PartitionSpec as P

CAP_FACTOR = 2
CHUNKS = 4
BLK = 256
LANE = 128
SUB = 8
STAGE = 512
F32 = jnp.float32
BF16 = jnp.bfloat16
SMEM = pl.BlockSpec(memory_space=pltpu.SMEM)
VMEM = pl.BlockSpec(memory_space=pltpu.VMEM)
HBM = pl.BlockSpec(memory_space=pl.ANY)
PARAMS = dict(vmem_limit_bytes=60 << 20)


def pipeline(body, n, in_specs=(), out_specs=()):
    return pltpu.emit_pipeline(lambda at, *refs: body(at.index[0], *refs), grid=(n,), in_specs=in_specs, out_specs=out_specs, _explicit_indices=True)


def dot(a, b):
    return jnp.dot(a, b, preferred_element_type=F32)


def dot_rt(a, b):
    return lax.dot_general(a, b, (((1,), (1,)), ((), ())), preferred_element_type=F32)


def dot_lt(a, b):
    return lax.dot_general(a, b, (((0,), (0,)), ((), ())), preferred_element_type=F32)


def lines_of(ref, row, n_groups):
    at = row * n_groups
    return ref[pl.ds(at, SUB), :], ref[pl.ds(at + SUB, n_groups - SUB), :]


def put_lines(ref, row, n_groups, val):
    at = row * n_groups
    ref[pl.ds(at, SUB), :] = val[0]
    ref[pl.ds(at + SUB, n_groups - SUB), :] = val[1]


def gather_kernel(chunk_tok, dim, slot_cap, n_dev, blk_e, blk_k, meta, slots, gsel, tok_hbm, *refs):
    x_out, dy_out, g_out, stage, rowbuf = refs[-5:]
    n_groups = dim // LANE
    off = meta[1]
    core = meta[2]
    half = n_dev // 2

    def clear(c, carry):
        stage[pl.ds(chunk_tok * n_groups + c, 1), :] = jnp.zeros((1, LANE), F32)
        return carry
    lax.fori_loop(0, n_groups, clear, 0)

    def fill(step, tok_ref):
        def convert(i, carry):
            at = (step * STAGE + i * 16) * n_groups
            for c in range(n_groups):
                val = tok_ref[pl.ds(pl.multiple_of(i * 16, 16), 16), c * LANE:(c + 1) * LANE].astype(F32)
                stage[pl.ds(at + c, SUB, stride=n_groups), :] = val[:SUB]
                stage[pl.ds(at + SUB * n_groups + c, SUB, stride=n_groups), :] = val[SUB:]
            return carry
        lax.fori_loop(0, STAGE // 16, convert, 0)

    def rows(b, rows_ref, *gate):
        e = blk_e[b]
        base = e * slot_cap + blk_k[b] * BLK

        def move(g, carry):
            vals = []
            for r in range(16):
                t = slots[base + g * 16 + r]
                vals.append(lines_of(stage, t, n_groups))
                if gate:
                    gate[0][pl.ds(g * 16 + r, 1), :] = jnp.full((1, LANE), gsel[e * chunk_tok + t], F32)
            for r in range(16):
                put_lines(rowbuf, g * 16 + r, n_groups, vals[r])
            return carry
        lax.fori_loop(0, BLK // 16, move, 0)

        def pack(i, carry):
            at = i * 16 * n_groups
            for c in range(n_groups):
                a = rowbuf[pl.ds(at + c, SUB, stride=n_groups), :]
                b2 = rowbuf[pl.ds(at + SUB * n_groups + c, SUB, stride=n_groups), :]
                rows_ref[pl.ds(pl.multiple_of(i * 16, 16), 16), c * LANE:(c + 1) * LANE] = jnp.concatenate([a, b2], axis=0).astype(BF16)
            return carry
        lax.fori_loop(0, BLK // 16, pack, 0)

    row_spec = pl.BlockSpec((BLK, dim), lambda i: (off + i, 0))
    gate_spec = pl.BlockSpec((BLK, LANE), lambda i: (off + i, 0))

    def fill_all(which):
        far = lambda i: i // half
        dev = lambda i: 2 * (i - half * far(i)) + core + far(i) * (1 - 2 * core)
        pipeline(fill, n_dev, in_specs=[pl.BlockSpec((STAGE, dim), lambda i: (2 * dev(i) + which, 0))])(tok_hbm)
    fill_all(0)
    pipeline(rows, meta[0], out_specs=[row_spec])(x_out)
    fill_all(1)
    pipeline(rows, meta[0], out_specs=[row_spec, gate_spec])(dy_out, g_out)


def gather_rows(tok, held, tables, n_rows, n_dev):
    chunk_tok, dim = tok.shape[0] // 2, tok.shape[1]
    slot_cap = tables[3].shape[0] // 8
    return pl.pallas_call(
        functools.partial(gather_kernel, chunk_tok, dim, slot_cap, n_dev),
        out_shape=[jax.ShapeDtypeStruct((n_rows, dim), BF16), jax.ShapeDtypeStruct((n_rows, dim), BF16), jax.ShapeDtypeStruct((n_rows, LANE), F32)],
        in_specs=[SMEM] * 5 + [HBM] * (1 + len(held)),
        out_specs=[HBM] * 3,
        scratch_shapes=[pltpu.VMEM(((chunk_tok + 2) * dim // LANE, LANE), F32), pltpu.VMEM((BLK * dim // LANE, LANE), F32)],
        input_output_aliases={6 + i: i for i in range(len(held))},
        compiler_params=pltpu.CompilerParams(**PARAMS),
        cost_estimate=pl.CostEstimate(flops=30_000_000_000, bytes_accessed=120_000_000, transcendentals=0),
        name="gather_rows",
    )(*tables, tok, *held)


def scale_rows(gate, dy):
    return jnp.concatenate([(gate * dy[:, c * LANE:(c + 1) * LANE]).astype(BF16) for c in range(dy.shape[1] // LANE)], axis=1)


def expert_body(e, x_ref, dy_ref, g_ref, w1_ref, w3_ref, w2_ref, o_ref, dx_ref, dg_ref, h_ref, d1_ref, d3_ref):
    x = x_ref[...]
    a1 = dot(x, w1_ref[0])
    a3 = dot(x, w3_ref[0])
    sig = jax.nn.sigmoid(a1)
    act = a1 * sig
    h = (act * a3).astype(BF16)
    h_ref[...] = h
    o = dot(h, w2_ref[0]).astype(BF16)
    o_ref[...] = o
    dy = dy_ref[...].astype(F32)
    prod = dy * o.astype(F32)
    part = prod[:, 0:LANE]
    for c in range(1, prod.shape[1] // LANE):
        part = part + prod[:, c * LANE:(c + 1) * LANE]
    dg = jnp.sum(part, axis=1, keepdims=True)
    lane = lax.broadcasted_iota(jnp.int32, part.shape, 1)
    dg_ref[...] = jnp.where(lane == e, dg, 0.0)
    dh = dot_rt(scale_rows(g_ref[...], dy), w2_ref[0])
    d1 = (dh * a3 * (sig * (1.0 + a1 * (1.0 - sig)))).astype(BF16)
    d3 = (dh * act).astype(BF16)
    d1_ref[...] = d1
    d3_ref[...] = d3
    dx_ref[...] = (dot_rt(d1, w1_ref[0]) + dot_rt(d3, w3_ref[0])).astype(BF16)


def expert_kernel(blk_e, meta, x, dy, g, w1, w3, w2, *refs):
    outs = refs[-6:]
    dim, ffn = w1.shape[1:]
    off = meta[1]
    glob = lambda i: (off + i, 0)
    loc = lambda i: (i, 0)
    wmap = lambda i: (blk_e[i], 0, 0)
    pipeline(
        lambda b, *refs: expert_body(blk_e[b], *refs), meta[0],
        in_specs=[pl.BlockSpec((BLK, dim), glob), pl.BlockSpec((BLK, dim), glob), pl.BlockSpec((BLK, LANE), glob),
                  pl.BlockSpec((1, dim, ffn), wmap), pl.BlockSpec((1, dim, ffn), wmap), pl.BlockSpec((1, ffn, dim), wmap)],
        out_specs=[pl.BlockSpec((BLK, dim), loc), pl.BlockSpec((BLK, dim), loc), pl.BlockSpec((BLK, LANE), loc)]
        + [pl.BlockSpec((BLK, ffn), glob)] * 3)(x, dy, g, w1, w3, w2, *outs)


def run_experts(x_rows, dy_rows, gates, w1, w3, w2, saved, blk_e, meta):
    n_rows, dim = x_rows.shape
    loc_rows = blk_e.shape[0] * BLK
    return pl.pallas_call(
        expert_kernel,
        out_shape=[jax.ShapeDtypeStruct((loc_rows, dim), BF16), jax.ShapeDtypeStruct((loc_rows, dim), BF16),
                   jax.ShapeDtypeStruct((loc_rows, LANE), F32)] + [jax.ShapeDtypeStruct((n_rows, w1.shape[2]), BF16)] * 3,
        in_specs=[SMEM] * 2 + [HBM] * (6 + len(saved)),
        out_specs=[HBM] * 6,
        input_output_aliases={8 + i: 3 + i for i in range(len(saved))},
        compiler_params=pltpu.CompilerParams(**PARAMS),
        cost_estimate=pl.CostEstimate(flops=55_000_000_000, bytes_accessed=80_000_000, transcendentals=0),
        name="experts",
    )(blk_e, meta, x_rows, dy_rows, gates, w1, w3, w2, *saved)


def combine_kernel(n_groups, slot_cap, blk_e, blk_k, meta, slots, o_hbm, g_hbm, dg_hbm, dx_hbm, keep_ref, send_ref, dgo_ref,
                   stage_y, stage_dx, stage_dg, rowbuf, sem):
    n_chip = keep_ref.shape[0]
    lines = keep_ref.shape[2]
    chunk_tok = 2 * n_chip * lines // n_groups
    dim = n_groups * LANE
    off = meta[1]

    def rows(stage, b, rows_ref, *gate):
        base = blk_e[b] * slot_cap + blk_k[b] * BLK

        def unpack(i, carry):
            at = i * 16 * n_groups
            rows16 = pl.ds(pl.multiple_of(i * 16, 16), 16)
            if gate:
                g16 = gate[0][rows16, :]
            for c in range(n_groups):
                val = rows_ref[rows16, c * LANE:(c + 1) * LANE].astype(F32)
                if gate:
                    val = val * g16
                rowbuf[pl.ds(at + c, SUB, stride=n_groups), :] = val[:SUB]
                rowbuf[pl.ds(at + SUB * n_groups + c, SUB, stride=n_groups), :] = val[SUB:]
            return carry
        lax.fori_loop(0, BLK // 16, unpack, 0)

        def add(g, carry):
            todo = []
            for r in range(SUB):
                t = slots[base + g * SUB + r]
                a, b2 = lines_of(rowbuf, g * SUB + r, n_groups)
                old_a, old_b = lines_of(stage, t, n_groups)
                more = (stage_dg[pl.ds(t, 1), :] + gate[1][pl.ds(g * SUB + r, 1), :],) if gate else ()
                todo.append((t, (old_a + a, old_b + b2), more))
            for t, val, more in todo:
                put_lines(stage, t, n_groups, val)
                if gate:
                    stage_dg[pl.ds(t, 1), :] = more[0]
            return carry
        lax.fori_loop(0, BLK // SUB, add, 0)

    def clear(stage, n):
        def zero(i, carry):
            for k in range(8):
                stage[pl.ds(pl.multiple_of(i * 64 + k * SUB, SUB), SUB), :] = jnp.zeros((SUB, LANE), F32)
            return carry
        lax.fori_loop(0, n // 64, zero, 0)

    def copies(stage, which):
        made = []
        for j in range(n_chip):
            made.append(pltpu.make_async_copy(stage.at[pl.ds(j * lines, lines)], keep_ref.at[j, which], sem.at[which]))
            made.append(pltpu.make_async_copy(stage.at[pl.ds((n_chip + j) * lines, lines)], send_ref.at[j, which], sem.at[which]))
        return made

    row_spec = pl.BlockSpec((BLK, dim), lambda i: (i, 0))
    clear(stage_y, chunk_tok * n_groups)
    clear(stage_dg, chunk_tok)
    pipeline(functools.partial(rows, stage_y), meta[0],
             in_specs=[row_spec, pl.BlockSpec((BLK, LANE), lambda i: (off + i, 0)), pl.BlockSpec((BLK, LANE), lambda i: (i, 0))])(o_hbm, g_hbm, dg_hbm)
    out_y = copies(stage_y, 0) + [pltpu.make_async_copy(stage_dg.at[pl.ds(0, chunk_tok)], dgo_ref, sem.at[2])]
    out_dx = copies(stage_dx, 1)
    for copy in out_y:
        copy.start()
    clear(stage_dx, chunk_tok * n_groups)
    pipeline(functools.partial(rows, stage_dx), meta[0], in_specs=[row_spec])(dx_hbm)
    for copy in out_dx:
        copy.start()
    for copy in out_y + out_dx:
        copy.wait()


def combine_rows(o_rows, gates, dg, dx_rows, tables, chunk_tok, n_chip):
    n_groups = o_rows.shape[1] // LANE
    slot_cap = tables[3].shape[0] // 8
    half = jax.ShapeDtypeStruct((n_chip, 2, chunk_tok * n_groups // (2 * n_chip), LANE), F32)
    stage = pltpu.VMEM(((chunk_tok + 2) * n_groups, LANE), F32)
    return pl.pallas_call(
        functools.partial(combine_kernel, n_groups, slot_cap),
        out_shape=[half, half, jax.ShapeDtypeStruct((chunk_tok, LANE), F32)],
        in_specs=[SMEM] * 4 + [HBM] * 4,
        out_specs=[HBM] * 3,
        scratch_shapes=[stage, stage, pltpu.VMEM((chunk_tok + SUB, LANE), F32), pltpu.VMEM((BLK * n_groups, LANE), F32), pltpu.SemaphoreType.DMA((3,))],
        compiler_params=pltpu.CompilerParams(**PARAMS),
        cost_estimate=pl.CostEstimate(flops=40_000_000_000, bytes_accessed=120_000_000, transcendentals=0),
        name="combine_rows",
    )(*tables[:4], o_rows, gates, dg, dx_rows)


def grad_kernel(order, owner, total, x, dy, g, h, d1, d3, o1, o3, o2, acc1, acc3, acc2):
    dim, ffn = o1.shape[1:]
    n = total[0]

    def step(i, x_ref, dy_ref, g_ref, h_ref, d1_ref, d3_ref, o1_ref, o3_ref, o2_ref):
        e = owner[i]
        first = jnp.logical_or(i == 0, owner[jnp.maximum(i - 1, 0)] != e)
        last = jnp.logical_or(i == n - 1, owner[jnp.minimum(i + 1, owner.shape[0] - 1)] != e)

        @pl.when(first)
        def _():
            acc1[...] = jnp.zeros_like(acc1)
            acc3[...] = jnp.zeros_like(acc3)
            acc2[...] = jnp.zeros_like(acc2)

        x = x_ref[...]
        acc1[...] += dot_lt(x, d1_ref[...])
        acc3[...] += dot_lt(x, d3_ref[...])
        acc2[...] += dot_lt(h_ref[...], scale_rows(g_ref[...], dy_ref[...].astype(F32)))

        @pl.when(last)
        def _():
            o1_ref[0] = acc1[...].astype(BF16)
            o3_ref[0] = acc3[...].astype(BF16)
            o2_ref[0] = acc2[...].astype(BF16)
    row = lambda i: (order[i], 0)
    wmap = lambda i: (owner[i], 0, 0)
    pipeline(
        step, n,
        in_specs=[pl.BlockSpec((BLK, dim), row), pl.BlockSpec((BLK, dim), row), pl.BlockSpec((BLK, LANE), row)]
        + [pl.BlockSpec((BLK, ffn), row)] * 3,
        out_specs=[pl.BlockSpec((1, dim, ffn), wmap), pl.BlockSpec((1, dim, ffn), wmap), pl.BlockSpec((1, ffn, dim), wmap)],
    )(x, dy, g, h, d1, d3, o1, o3, o2)


def weight_grads(x_rows, dy_rows, gates, saved, order, owner, total, n_local):
    dim = x_rows.shape[1]
    ffn = saved[0].shape[1]
    return pl.pallas_call(
        grad_kernel,
        out_shape=[jax.ShapeDtypeStruct((n_local, dim, ffn), BF16), jax.ShapeDtypeStruct((n_local, dim, ffn), BF16),
                   jax.ShapeDtypeStruct((n_local, ffn, dim), BF16)],
        in_specs=[SMEM] * 3 + [HBM] * 6,
        out_specs=[HBM] * 3,
        scratch_shapes=[pltpu.VMEM((dim, ffn), F32), pltpu.VMEM((dim, ffn), F32), pltpu.VMEM((ffn, dim), F32)],
        compiler_params=pltpu.CompilerParams(**PARAMS),
        cost_estimate=pl.CostEstimate(flops=100_000_000_000, bytes_accessed=160_000_000, transcendentals=0),
        name="weight_grads",
    )(order, owner, total, x_rows, dy_rows, gates, *saved)


def shared_kernel(n_arr, n_dev, place, *refs):
    toks = refs[:n_arr]
    w1_ref, w3_ref, w2_ref, o1_ref, o3_ref, o2_ref, near_ref, far_ref, xbuf, dybuf, hbuf, d1buf, d3buf, outbuf, sem, out_sem = refs[n_arr:]
    total = n_arr * n_dev
    me = place[0]
    chip = me // 2

    def copies(k, dev, slot):
        return (pltpu.make_async_copy(toks[k].at[pl.ds(2 * dev * STAGE, STAGE)], xbuf.at[slot], sem.at[slot, 0]),
                pltpu.make_async_copy(toks[k].at[pl.ds((2 * dev + 1) * STAGE, STAGE)], dybuf.at[slot], sem.at[slot, 1]))

    def fetch(i, slot):
        which = i // n_dev
        for k in range(n_arr):
            @pl.when(which == k)
            def _():
                for copy in copies(k, i - which * n_dev, slot):
                    copy.start()

    def put(ref, which):
        return pltpu.make_async_copy(outbuf, ref.at[:, pl.ds(which * STAGE, STAGE)], out_sem)

    fetch(0, 0)
    o1_ref[...] = jnp.zeros_like(o1_ref)
    o3_ref[...] = jnp.zeros_like(o3_ref)
    o2_ref[...] = jnp.zeros_like(o2_ref)

    def step(i, carry):
        slot = lax.rem(i, 2)
        which = i // n_dev
        dev = i - which * n_dev

        @pl.when(i + 1 < total)
        def _():
            fetch(i + 1, 1 - slot)
        for copy in copies(0, 0, slot):
            copy.wait()
        x = xbuf[slot]
        dy = dybuf[slot]
        b1 = dot(x, w1_ref[...])
        b3 = dot(x, w3_ref[...])
        sig = jax.nn.sigmoid(b1)
        act = b1 * sig
        h = (act * b3).astype(BF16)
        hbuf[...] = h
        o2_ref[...] += dot_lt(h, dy)
        dh = dot_rt(dy, w2_ref[...])
        d1 = (dh * b3 * (sig * (1.0 + b1 * (1.0 - sig)))).astype(BF16)
        d1buf[...] = d1
        o1_ref[...] += dot_lt(x, d1)
        d3 = (dh * act).astype(BF16)
        d3buf[...] = d3
        o3_ref[...] += dot_lt(x, d3)

        @pl.when(dev // 2 == chip)
        def _():
            outbuf[0] = dot(hbuf[...], w2_ref[...])
            outbuf[1] = dot_rt(d1buf[...], w1_ref[...]) + dot_rt(d3buf[...], w3_ref[...])

            @pl.when(dev == me)
            def _():
                put(near_ref, which).start()

            @pl.when(dev != me)
            def _():
                put(far_ref, which).start()
            put(near_ref, 0).wait()
        return carry
    lax.fori_loop(0, total, step, 0)


def shared_half(toks, w1, w3, w2, me, n_dev):
    dim, width = w1.shape
    part = jax.ShapeDtypeStruct((2, len(toks) * STAGE, dim), F32)
    small = pltpu.VMEM((STAGE, width), BF16)
    return pl.pallas_call(
        functools.partial(shared_kernel, len(toks), n_dev),
        out_shape=[jax.ShapeDtypeStruct((dim, width), F32), jax.ShapeDtypeStruct((dim, width), F32), jax.ShapeDtypeStruct((width, dim), F32), part, part],
        in_specs=[SMEM] + [HBM] * len(toks) + [VMEM] * 3,
        out_specs=[VMEM] * 3 + [HBM] * 2,
        scratch_shapes=[pltpu.VMEM((2, STAGE, dim), BF16), pltpu.VMEM((2, STAGE, dim), BF16), small, small, small,
                        pltpu.VMEM((2, STAGE, dim), F32), pltpu.SemaphoreType.DMA((2, 2)), pltpu.SemaphoreType.DMA],
        compiler_params=pltpu.CompilerParams(**PARAMS),
        cost_estimate=pl.CostEstimate(flops=170_000_000_000, bytes_accessed=160_000_000, transcendentals=0),
        name="shared_half",
    )(me[None], *toks, w1, w3, w2)


def finish_kernel(n_groups, sum_ref, near_ref, got_ref, *refs):
    y_ref, dx_ref = refs[-2:]

    def body(i, carry):
        rows16 = pl.ds(pl.multiple_of(i * 16, 16), 16)
        at = i * 16 * n_groups
        for which, out in ((0, y_ref), (1, dx_ref)):
            for c in range(n_groups):
                lanes = slice(c * LANE, (c + 1) * LANE)
                a = sum_ref[0, which, pl.ds(at + c, SUB, stride=n_groups), :]
                b = sum_ref[0, which, pl.ds(at + SUB * n_groups + c, SUB, stride=n_groups), :]
                val = jnp.concatenate([a, b], axis=0) + (near_ref[which, rows16, lanes] + got_ref[which, rows16, lanes])
                out[rows16, lanes] = val.astype(BF16)
        return carry
    lax.fori_loop(0, y_ref.shape[0] // 16, body, 0)


def finish(chunk, sums, near, got, held):
    n_tok, dim = near.shape[1:]
    n_groups = dim // LANE
    part = sums.shape[2] // n_groups
    row = pl.BlockSpec((part // 2, dim), lambda i: (2 * chunk + i, 0))
    both = pl.BlockSpec((2, part // 2, dim), lambda i: (0, 2 * chunk + i, 0))
    return pl.pallas_call(
        functools.partial(finish_kernel, n_groups),
        out_shape=[jax.ShapeDtypeStruct((n_tok, dim), BF16)] * 2,
        grid=(2,),
        in_specs=[pl.BlockSpec((1, 2, sums.shape[2] // 2, LANE), lambda i: (0, 0, i, 0)), both, both] + [HBM] * len(held),
        out_specs=[row, row],
        input_output_aliases={3 + i: i for i in range(len(held))},
        compiler_params=pltpu.CompilerParams(dimension_semantics=("arbitrary",), **PARAMS),
        cost_estimate=pl.CostEstimate(flops=4_000_000_000, bytes_accessed=20_000_000, transcendentals=0),
        name="finish",
    )(sums, near, got, *held)


def route(ids_all, gates_all, first_expert, n_local, slot_cap):
    n_chunk, n_top, chunk_tok = ids_all.shape
    experts = first_expert + jnp.arange(n_local, dtype=jnp.int32)
    match = ids_all[:, None] == experts[None, :, None, None]
    hit = jnp.any(match, axis=2)
    gsel = jnp.sum(jnp.where(match, gates_all[:, None], 0.0), axis=2)
    n_seg = chunk_tok // LANE
    strict = (jnp.arange(LANE)[:, None] < jnp.arange(LANE)[None, :]).astype(BF16)
    seg = hit.reshape(n_chunk, n_local, n_seg, LANE)
    inner = jnp.einsum('cesl,lm->cesm', seg.astype(BF16), strict, preferred_element_type=F32)
    seg_sum = jnp.sum(seg, axis=3, dtype=jnp.int32)
    before = jnp.arange(n_seg)[:, None] < jnp.arange(n_seg)[None, :]
    outer = jnp.sum(jnp.where(before, seg_sum[..., :, None], 0), axis=2)
    rank = (inner.astype(jnp.int32) + outer[..., None]).reshape(n_chunk, n_local, chunk_tok)
    count = jnp.sum(seg_sum, axis=2)
    n_hi = slot_cap // 64
    hi = jnp.where(hit, rank >> 6, -1)
    lo = rank & 63
    pick_hi = (hi[:, :, None, :] == jnp.arange(n_hi, dtype=jnp.int32)[:, None]).astype(BF16)
    tok = jnp.arange(chunk_tok, dtype=jnp.int32)
    pick_lo = lo[:, :, None, :] == jnp.arange(64, dtype=jnp.int32)[:, None]
    val_lo = jnp.concatenate([jnp.where(pick_lo, (tok >> 6), 0), jnp.where(pick_lo, (tok & 63), 0)], axis=2).astype(BF16)
    found = jnp.einsum('ceht,cent->cehn', pick_hi, val_lo, preferred_element_type=F32).astype(jnp.int32)
    slots = (found[..., :64] * 64 + found[..., 64:]).reshape(n_chunk, n_local, slot_cap)
    slots = jnp.where(jnp.arange(slot_cap, dtype=jnp.int32) < count[..., None], slots, chunk_tok)
    n_blk = (count + BLK - 1) // BLK
    upto = jnp.cumsum(n_blk, axis=1)
    chunk_blk = upto[:, -1]
    chunk_off = jnp.cumsum(chunk_blk) - chunk_blk
    max_blk = n_local * (slot_cap // BLK)
    at = jnp.arange(max_blk, dtype=jnp.int32)
    blk_e = jnp.minimum(jnp.sum(at[None, :, None] >= upto[:, None, :], axis=2, dtype=jnp.int32), n_local - 1)
    start = upto - n_blk
    blk_k = at[None, :] - jnp.sum(jnp.where(blk_e[..., None] == jnp.arange(n_local), start[:, None, :], 0), axis=2)
    glob = (chunk_off[:, None] + start).T.reshape(-1)
    cnt = n_blk.T.reshape(-1)
    end = jnp.cumsum(cnt)
    total_blk = end[-1]
    at2 = jnp.arange(n_local * slot_cap // BLK + n_chunk * n_local, dtype=jnp.int32)
    grp = jnp.minimum(jnp.sum(at2[:, None] >= end[None, :], axis=1, dtype=jnp.int32), cnt.shape[0] - 1)
    sel = grp[:, None] == jnp.arange(cnt.shape[0])
    order = at2 + jnp.sum(jnp.where(sel, (glob - (end - cnt))[None, :], 0), axis=1)
    order = jnp.clip(order, 0, at2.shape[0] - 1).astype(jnp.int32)
    owner = (grp // n_chunk).astype(jnp.int32)
    return slots, gsel, blk_e, blk_k.astype(jnp.int32), chunk_blk, chunk_off, order, owner, total_blk


def solution(mesh):
    ei_size = mesh.shape['ei']
    ex_size = mesh.shape['eo'] // 2
    n_chip = ei_size * ex_size
    group_size = 2 * n_chip
    split_mesh = jax.sharding.Mesh(mesh.devices.reshape(mesh.shape['dp'], ei_size, ex_size, 2), ('dp', 'ei', 'ex', 'core'))
    axes = ('ei', 'ex', 'core')
    chips = ('ei', 'ex')
    tok_spec = P(('dp', *axes), None)
    exp_spec = P(axes, None, None)
    full_spec = P(None, None)
    grad_spec = P(('dp', *axes), None, None)
    shared_spec = P('dp', None)

    def swap(v):
        return lax.ppermute(v, 'core', [(0, 1), (1, 0)])

    def device_step(x_loc, ids_loc, gates_loc, w_one, w_three, w_two, s_one, s_three, s_two, dy_loc):
        n_tok, n_top = ids_loc.shape
        dim = x_loc.shape[1]
        n_local = w_one.shape[0]
        n_exp = n_local * group_size
        cap = min(n_tok, CAP_FACTOR * ((n_tok * n_top + n_exp - 1) // n_exp))
        slot_cap = cap * group_size
        part = n_tok // CHUNKS
        chunk_tok = part * group_size
        core = lax.axis_index('core')
        me = (lax.axis_index('ei') * ex_size + lax.axis_index('ex')) * 2 + core

        mine = [jnp.concatenate([v[c * part:(c + 1) * part] for v in (x_loc, dy_loc)]) for c in range(CHUNKS)]
        toks = [lax.all_gather(v, axes, axis=0, tiled=True) for v in lax.optimization_barrier(mine)]

        def near_first(v, axis):
            return jnp.where(core == 0, v, jnp.flip(v, axis))

        both = lax.all_gather(jnp.concatenate([ids_loc.T.astype(F32), gates_loc.T]), axes, axis=0)
        both = near_first(both.reshape(n_chip, 2, 2 * n_top, CHUNKS, part), 1).transpose(3, 2, 1, 0, 4).reshape(CHUNKS, 2 * n_top, chunk_tok)
        slots, gsel, blk_e, blk_k, chunk_blk, chunk_off, order, owner, total_blk = route(
            both[:, :n_top].astype(jnp.int32), both[:, n_top:], me * n_local, n_local, slot_cap)
        n_rows = order.shape[0] * BLK

        held, saved = [], []
        sums, dg_parts = [], []
        for c in range(CHUNKS):
            meta = jnp.stack([chunk_blk[c], chunk_off[c], core]).astype(jnp.int32)
            gpad = jnp.concatenate([gsel[c].reshape(-1), jnp.zeros((LANE,), F32)])
            tables = (blk_e[c], blk_k[c], meta, slots[c].reshape(-1), gpad)
            x_rows, dy_rows, gate_rows = gather_rows(toks[c], held, tables, n_rows, group_size)
            if c > 0:
                x_rows, keep, theirs = lax.optimization_barrier((x_rows, keep, theirs))
                sums.append(lax.psum_scatter(keep + theirs, chips, scatter_dimension=0, tiled=True))
            o_rows, dx_rows, dg, *saved = run_experts(x_rows, dy_rows, gate_rows, w_one, w_three, w_two, saved, blk_e[c], meta)
            keep, send, dg_part = combine_rows(o_rows, gate_rows, dg, dx_rows, tables, chunk_tok, n_chip)
            theirs = swap(send)
            held = [x_rows, dy_rows, gate_rows]
            dg_parts.append(dg_part[:, :n_local].T.reshape(n_local, 2, n_chip, part))
        sums.append(lax.psum_scatter(keep + theirs, chips, scatter_dimension=0, tiled=True))
        dw_one, dw_three, dw_two = weight_grads(x_rows, dy_rows, gate_rows, saved, order, owner, total_blk[None], n_local)

        width = s_one.shape[1] // 2
        toks, dw_one = lax.optimization_barrier((toks, dw_one))
        *halves, near, far = shared_half(toks, lax.dynamic_slice_in_dim(s_one, core * width, width, 1), lax.dynamic_slice_in_dim(s_three, core * width, width, 1),
                                         lax.dynamic_slice_in_dim(s_two, core * width, width, 0), me, group_size)
        got = swap(far)

        def join(mine, axis):
            theirs = swap(mine)
            return jnp.concatenate([jnp.where(core == 0, mine, theirs), jnp.where(core == 0, theirs, mine)], axis=axis)
        dws_one, dws_three, dws_two = join(halves[0], 1), join(halves[1], 1), join(halves[2], 0)

        dg_send = near_first(jnp.stack(dg_parts, axis=1), 2).transpose(3, 2, 0, 1, 4)
        dg_recv = lax.all_to_all(dg_send.reshape(group_size, n_local, n_tok), axes, 0, 0)
        dg_tok = dg_recv.reshape(n_exp, n_tok)
        pick = ids_loc.T[:, None, :] == jnp.arange(n_exp, dtype=jnp.int32)[:, None]
        d_gates = jnp.sum(jnp.where(pick, dg_tok[None], 0.0), axis=1).T

        outs = []
        for c in range(CHUNKS):
            outs = finish(c, sums[c], near, got, outs)
        y_loc, dx_loc = outs
        return (y_loc, dx_loc, d_gates, dw_one, dw_three, dw_two, dws_one, dws_three, dws_two)

    return jax.shard_map(device_step, mesh=split_mesh, in_specs=(tok_spec, tok_spec, tok_spec, exp_spec, exp_spec, exp_spec, full_spec, full_spec, full_spec, tok_spec), out_specs=(tok_spec, tok_spec, tok_spec, grad_spec, grad_spec, grad_spec, shared_spec, shared_spec, shared_spec), check_vma=False)
```

```python
import functools

import jax
import jax.numpy as jnp
from jax import lax
from jax.experimental import pallas as pl
from jax.experimental.pallas import tpu as pltpu
from jax.sharding import PartitionSpec as P


CAP_FACTOR = 2
CHUNKS = 4
PER_GATHER = 2
SCATTERS = ((0,), (1, 2), (3,))
BLK = 512
LANE = 128
SUB = 8
STAGE = 512
F32 = jnp.float32
BF16 = jnp.bfloat16
SMEM = pl.BlockSpec(memory_space=pltpu.SMEM)
VMEM = pl.BlockSpec(memory_space=pltpu.VMEM)
HBM = pl.BlockSpec(memory_space=pl.ANY)
PARAMS = dict(vmem_limit_bytes=60 << 20)


def pipeline(body, n, in_specs=(), out_specs=()):
    return pltpu.emit_pipeline(lambda at, *refs: body(at.index[0], *refs), grid=(n,), in_specs=in_specs, out_specs=out_specs, _explicit_indices=True)


def dot(a, b):
    return jnp.dot(a, b, preferred_element_type=F32)


def dot_rt(a, b):
    return lax.dot_general(a, b, (((1,), (1,)), ((), ())), preferred_element_type=F32)


def dot_lt(a, b):
    return lax.dot_general(a, b, (((0,), (0,)), ((), ())), preferred_element_type=F32)


def lines_of(ref, row, n_groups):
    at = row * n_groups
    return ref[pl.ds(at, SUB), :], ref[pl.ds(at + SUB, n_groups - SUB), :]


def put_lines(ref, row, n_groups, val):
    at = row * n_groups
    ref[pl.ds(at, SUB), :] = val[0]
    ref[pl.ds(at + SUB, n_groups - SUB), :] = val[1]


def gather_kernel(chunk, chunk_tok, dim, slot_cap, n_dev, blk_e, blk_k, blk_n, meta, slots, gsel, tok_hbm, *refs):
    x_out, dy_out, g_out, stage, rowbuf = refs[-5:]
    n_groups = dim // LANE
    off = meta[1]
    core = meta[2]
    half = n_dev // 2

    def clear(c, carry):
        stage[pl.ds(chunk_tok * n_groups + c, 1), :] = jnp.zeros((1, LANE), F32)
        return carry
    lax.fori_loop(0, n_groups, clear, 0)

    def fill(step, tok_ref):
        def convert(i, carry):
            at = (step * STAGE + i * 16) * n_groups
            for c in range(n_groups):
                val = tok_ref[pl.ds(pl.multiple_of(i * 16, 16), 16), c * LANE:(c + 1) * LANE].astype(F32)
                stage[pl.ds(at + c, SUB, stride=n_groups), :] = val[:SUB]
                stage[pl.ds(at + SUB * n_groups + c, SUB, stride=n_groups), :] = val[SUB:]
            return carry
        lax.fori_loop(0, STAGE // 16, convert, 0)

    def rows(b, rows_ref, *gate):
        e = blk_e[b]
        base = e * slot_cap + blk_k[b] * BLK
        n_used = pl.cdiv(jnp.minimum(blk_n[b], BLK), 16)

        def move(g, carry):
            vals = []
            for r in range(16):
                t = slots[base + g * 16 + r]
                vals.append(lines_of(stage, t, n_groups))
                if gate:
                    gate[0][pl.ds(g * 16 + r, 1), :] = jnp.full((1, LANE), gsel[e * chunk_tok + t], F32)
            for r in range(16):
                put_lines(rowbuf, g * 16 + r, n_groups, vals[r])
            return carry
        lax.fori_loop(0, n_used, move, 0)

        def pack(i, carry):
            at = i * 16 * n_groups
            for c in range(n_groups):
                a = rowbuf[pl.ds(at + c, SUB, stride=n_groups), :]
                b2 = rowbuf[pl.ds(at + SUB * n_groups + c, SUB, stride=n_groups), :]
                rows_ref[pl.ds(pl.multiple_of(i * 16, 16), 16), c * LANE:(c + 1) * LANE] = jnp.concatenate([a, b2], axis=0).astype(BF16)
            return carry
        lax.fori_loop(0, n_used, pack, 0)

        def blank(i, carry):
            rows16 = pl.ds(pl.multiple_of(i * 16, 16), 16)
            rows_ref[rows16, :] = jnp.zeros((16, dim), BF16)
            if gate:
                gate[0][rows16, :] = jnp.zeros((16, LANE), F32)
            return carry
        lax.fori_loop(n_used, BLK // 16, blank, 0)

    row_spec = pl.BlockSpec((BLK, dim), lambda i: (off + i, 0))
    gate_spec = pl.BlockSpec((BLK, LANE), lambda i: (off + i, 0))

    def fill_all(which):
        far = lambda i: i // half
        dev = lambda i: 2 * (i - half * far(i)) + core + far(i) * (1 - 2 * core)
        row = lambda i: ((dev(i) * 2 + which) * PER_GATHER + chunk, 0)
        pipeline(fill, n_dev, in_specs=[pl.BlockSpec((STAGE, dim), row)])(tok_hbm)
    fill_all(0)
    pipeline(rows, meta[0], out_specs=[row_spec])(x_out)
    fill_all(1)
    pipeline(rows, meta[0], out_specs=[row_spec, gate_spec])(dy_out, g_out)


def gather_rows(chunk, tok, held, tables, n_rows, n_dev):
    dim = tok.shape[1]
    chunk_tok = STAGE * n_dev
    slot_cap = tables[4].shape[0] // 8
    return pl.pallas_call(
        functools.partial(gather_kernel, chunk, chunk_tok, dim, slot_cap, n_dev),
        out_shape=[jax.ShapeDtypeStruct((n_rows, dim), BF16), jax.ShapeDtypeStruct((n_rows, dim), BF16), jax.ShapeDtypeStruct((n_rows, LANE), F32)],
        in_specs=[SMEM] * 6 + [HBM] * (1 + len(held)),
        out_specs=[HBM] * 3,
        scratch_shapes=[pltpu.VMEM(((chunk_tok + 2) * dim // LANE, LANE), F32), pltpu.VMEM((BLK * dim // LANE, LANE), F32)],
        input_output_aliases={7 + i: i for i in range(len(held))},
        compiler_params=pltpu.CompilerParams(**PARAMS),
        cost_estimate=pl.CostEstimate(flops=30_000_000_000, bytes_accessed=120_000_000, transcendentals=0),
        name="gather_rows",
    )(*tables, tok, *held)


def scale_rows(gate, dy):
    return jnp.concatenate([(gate * dy[:, c * LANE:(c + 1) * LANE]).astype(BF16) for c in range(dy.shape[1] // LANE)], axis=1)


def expert_body(e, x_ref, dy_ref, g_ref, w1_ref, w3_ref, w2_ref, o_ref, dx_ref, dg_ref, h_ref, d1_ref, d3_ref):
    x = x_ref[...]
    a1 = dot(x, w1_ref[0])
    a3 = dot(x, w3_ref[0])
    sig = jax.nn.sigmoid(a1)
    act = a1 * sig
    h = (act * a3).astype(BF16)
    h_ref[...] = h
    o = dot(h, w2_ref[0]).astype(BF16)
    o_ref[...] = o
    dy = dy_ref[...].astype(F32)
    prod = dy * o.astype(F32)
    part = prod[:, 0:LANE]
    for c in range(1, prod.shape[1] // LANE):
        part = part + prod[:, c * LANE:(c + 1) * LANE]
    dg = jnp.sum(part, axis=1, keepdims=True)
    lane = lax.broadcasted_iota(jnp.int32, part.shape, 1)
    dg_ref[...] = jnp.where(lane == e, dg, 0.0)
    dh = dot_rt(scale_rows(g_ref[...], dy), w2_ref[0])
    d1 = (dh * a3 * (sig * (1.0 + a1 * (1.0 - sig)))).astype(BF16)
    d3 = (dh * act).astype(BF16)
    d1_ref[...] = d1
    d3_ref[...] = d3
    dx_ref[...] = (dot_rt(d1, w1_ref[0]) + dot_rt(d3, w3_ref[0])).astype(BF16)


def expert_kernel(blk_e, meta, x, dy, g, w1, w3, w2, *refs):
    outs = refs[-6:]
    dim, ffn = w1.shape[1:]
    off = meta[1]
    glob = lambda i: (off + i, 0)
    loc = lambda i: (i, 0)
    wmap = lambda i: (blk_e[i], 0, 0)
    pipeline(
        lambda b, *refs: expert_body(blk_e[b], *refs), meta[0],
        in_specs=[pl.BlockSpec((BLK, dim), glob), pl.BlockSpec((BLK, dim), glob), pl.BlockSpec((BLK, LANE), glob),
                  pl.BlockSpec((1, dim, ffn), wmap), pl.BlockSpec((1, dim, ffn), wmap), pl.BlockSpec((1, ffn, dim), wmap)],
        out_specs=[pl.BlockSpec((BLK, dim), loc), pl.BlockSpec((BLK, dim), loc), pl.BlockSpec((BLK, LANE), loc)]
        + [pl.BlockSpec((BLK, ffn), glob)] * 3)(x, dy, g, w1, w3, w2, *outs)


def run_experts(x_rows, dy_rows, gates, w1, w3, w2, saved, blk_e, meta):
    n_rows, dim = x_rows.shape
    loc_rows = blk_e.shape[0] * BLK
    return pl.pallas_call(
        expert_kernel,
        out_shape=[jax.ShapeDtypeStruct((loc_rows, dim), BF16), jax.ShapeDtypeStruct((loc_rows, dim), BF16),
                   jax.ShapeDtypeStruct((loc_rows, LANE), F32)] + [jax.ShapeDtypeStruct((n_rows, w1.shape[2]), BF16)] * 3,
        in_specs=[SMEM] * 2 + [HBM] * (6 + len(saved)),
        out_specs=[HBM] * 6,
        input_output_aliases={8 + i: 3 + i for i in range(len(saved))},
        compiler_params=pltpu.CompilerParams(**PARAMS),
        cost_estimate=pl.CostEstimate(flops=55_000_000_000, bytes_accessed=80_000_000, transcendentals=0),
        name="experts",
    )(blk_e, meta, x_rows, dy_rows, gates, w1, w3, w2, *saved)


def combine_kernel(far, where, n_groups, slot_cap, blk_e, blk_k, blk_n, blk_near, meta, slots, o_hbm, g_hbm, dg_hbm, dx_hbm, *refs):
    out_ref, dgo_ref, stage_y, stage_dx, stage_dg, rowbuf, sem = refs[-7:]
    n_chip = out_ref.shape[0]
    lines = out_ref.shape[3]
    half = n_chip * lines // n_groups
    dim = n_groups * LANE
    off = meta[1]

    def rows(stage, b, rows_ref, *gate):
        base = blk_e[b] * slot_cap + blk_k[b] * BLK
        near = jnp.minimum(blk_near[b], BLK)
        if far:
            first, last = near, jnp.minimum(blk_n[b], BLK)
        else:
            first, last = 0, near

        def unpack(i, carry):
            at = i * 16 * n_groups
            rows16 = pl.ds(pl.multiple_of(i * 16, 16), 16)
            if gate:
                g16 = gate[0][rows16, :]
            for c in range(n_groups):
                val = rows_ref[rows16, c * LANE:(c + 1) * LANE].astype(F32)
                if gate:
                    val = val * g16
                rowbuf[pl.ds(at + c, SUB, stride=n_groups), :] = val[:SUB]
                rowbuf[pl.ds(at + SUB * n_groups + c, SUB, stride=n_groups), :] = val[SUB:]
            return carry
        lax.fori_loop(first // 16, pl.cdiv(last, 16), unpack, 0)

        def add(g, carry):
            todo = []
            for r in range(SUB):
                t = slots[base + g * SUB + r]
                if far:
                    t = t - half
                    t = jnp.where(t < 0, half, t)
                else:
                    t = jnp.minimum(t, half)
                a, b2 = lines_of(rowbuf, g * SUB + r, n_groups)
                old_a, old_b = lines_of(stage, t, n_groups)
                more = (stage_dg[pl.ds(t, 1), :] + gate[1][pl.ds(g * SUB + r, 1), :],) if gate else ()
                todo.append((t, (old_a + a, old_b + b2), more))
            for t, val, more in todo:
                put_lines(stage, t, n_groups, val)
                if gate:
                    stage_dg[pl.ds(t, 1), :] = more[0]
            return carry

        @pl.when(last > first)
        def _():
            lax.fori_loop(first // SUB, pl.cdiv(last, SUB), add, 0)

    def clear(stage, n):
        def zero(i, carry):
            for k in range(8):
                stage[pl.ds(pl.multiple_of(i * 64 + k * SUB, SUB), SUB), :] = jnp.zeros((SUB, LANE), F32)
            return carry
        lax.fori_loop(0, n // 64, zero, 0)

    def loads(stage, which):
        return [pltpu.make_async_copy(refs[0].at[j, 0, which], stage.at[pl.ds(j * lines, lines)], sem.at[3 + which]) for j in range(n_chip)]

    def stores(stage, which):
        return [pltpu.make_async_copy(stage.at[pl.ds(j * lines, lines)], out_ref.at[j, where, which], sem.at[which]) for j in range(n_chip)]

    def start(copies):
        for copy in copies:
            copy.start()

    def wait(copies):
        for copy in copies:
            copy.wait()

    row_spec = pl.BlockSpec((BLK, dim), lambda i: (i, 0))
    if not far:
        start(loads(stage_y, 0))
        start(loads(stage_dx, 1))
    clear(stage_dg, half)
    if far:
        clear(stage_y, half * n_groups)
    else:
        wait(loads(stage_y, 0))
    pipeline(functools.partial(rows, stage_y), meta[0],
             in_specs=[row_spec, pl.BlockSpec((BLK, LANE), lambda i: (off + i, 0)), pl.BlockSpec((BLK, LANE), lambda i: (i, 0))])(o_hbm, g_hbm, dg_hbm)
    out = stores(stage_y, 0) + [pltpu.make_async_copy(stage_dg.at[pl.ds(0, half)], dgo_ref, sem.at[2])]
    start(out)
    if far:
        clear(stage_dx, half * n_groups)
    else:
        wait(loads(stage_dx, 1))
    pipeline(functools.partial(rows, stage_dx), meta[0], in_specs=[row_spec])(dx_hbm)
    start(stores(stage_dx, 1))
    wait(out + stores(stage_dx, 1))


def combine_rows(o_rows, gates, dg, dx_rows, tables, chunk_tok, n_chip, theirs, where=0, n_held=1, held=None):
    n_groups = o_rows.shape[1] // LANE
    blk_e, blk_k, blk_n, blk_near, meta, slots, _ = tables
    half = chunk_tok // 2
    more = [] if theirs is None else [theirs]
    more += [] if held is None else [held]
    stage = pltpu.VMEM(((half + 2) * n_groups, LANE), F32)
    return pl.pallas_call(
        functools.partial(combine_kernel, theirs is None, where, n_groups, slots.shape[0] // 8),
        out_shape=[jax.ShapeDtypeStruct((n_chip, n_held, 2, half * n_groups // n_chip, LANE), F32), jax.ShapeDtypeStruct((half, LANE), F32)],
        in_specs=[SMEM] * 6 + [HBM] * (4 + len(more)),
        out_specs=[HBM] * 2,
        input_output_aliases={} if held is None else {11: 0},
        scratch_shapes=[stage, stage, pltpu.VMEM((half + SUB, LANE), F32), pltpu.VMEM((BLK * n_groups, LANE), F32), pltpu.SemaphoreType.DMA((5,))],
        compiler_params=pltpu.CompilerParams(**PARAMS),
        cost_estimate=pl.CostEstimate(flops=20_000_000_000, bytes_accessed=60_000_000, transcendentals=0),
        name="combine_far" if theirs is None else "combine_near",
    )(blk_e, blk_k, blk_n, blk_near, meta, slots, o_rows, gates, dg, dx_rows, *more)


def grad_kernel(order, owner, total, x, dy, g, h, d1, d3, o1, o3, o2, acc1, acc3, acc2):
    dim, ffn = o1.shape[1:]
    n = total[0]

    def step(i, x_ref, dy_ref, g_ref, h_ref, d1_ref, d3_ref, o1_ref, o3_ref, o2_ref):
        e = owner[i]
        first = jnp.logical_or(i == 0, owner[jnp.maximum(i - 1, 0)] != e)
        last = jnp.logical_or(i == n - 1, owner[jnp.minimum(i + 1, owner.shape[0] - 1)] != e)

        @pl.when(first)
        def _():
            acc1[...] = jnp.zeros_like(acc1)
            acc3[...] = jnp.zeros_like(acc3)
            acc2[...] = jnp.zeros_like(acc2)

        x = x_ref[...]
        acc1[...] += dot_lt(x, d1_ref[...])
        acc3[...] += dot_lt(x, d3_ref[...])
        acc2[...] += dot_lt(h_ref[...], scale_rows(g_ref[...], dy_ref[...].astype(F32)))

        @pl.when(last)
        def _():
            o1_ref[0] = acc1[...].astype(BF16)
            o3_ref[0] = acc3[...].astype(BF16)
            o2_ref[0] = acc2[...].astype(BF16)
    row = lambda i: (order[i], 0)
    wmap = lambda i: (owner[i], 0, 0)
    pipeline(
        step, n,
        in_specs=[pl.BlockSpec((BLK, dim), row), pl.BlockSpec((BLK, dim), row), pl.BlockSpec((BLK, LANE), row)]
        + [pl.BlockSpec((BLK, ffn), row)] * 3,
        out_specs=[pl.BlockSpec((1, dim, ffn), wmap), pl.BlockSpec((1, dim, ffn), wmap), pl.BlockSpec((1, ffn, dim), wmap)],
    )(x, dy, g, h, d1, d3, o1, o3, o2)


def weight_grads(x_rows, dy_rows, gates, saved, order, owner, total, n_local):
    dim = x_rows.shape[1]
    ffn = saved[0].shape[1]
    return pl.pallas_call(
        grad_kernel,
        out_shape=[jax.ShapeDtypeStruct((n_local, dim, ffn), BF16), jax.ShapeDtypeStruct((n_local, dim, ffn), BF16),
                   jax.ShapeDtypeStruct((n_local, ffn, dim), BF16)],
        in_specs=[SMEM] * 3 + [HBM] * 6,
        out_specs=[HBM] * 3,
        scratch_shapes=[pltpu.VMEM((dim, ffn), F32), pltpu.VMEM((dim, ffn), F32), pltpu.VMEM((ffn, dim), F32)],
        compiler_params=pltpu.CompilerParams(**PARAMS),
        cost_estimate=pl.CostEstimate(flops=100_000_000_000, bytes_accessed=160_000_000, transcendentals=0),
        name="weight_grads",
    )(order, owner, total, x_rows, dy_rows, gates, *saved)


def shared_kernel(n_arr, n_dev, place, *refs):
    toks = refs[:n_arr]
    w1_ref, w3_ref, w2_ref, o1_ref, o3_ref, o2_ref, near_ref, far_ref, xbuf, dybuf, hbuf, d1buf, d3buf, outbuf, sem, out_sem = refs[n_arr:]
    total = n_arr * PER_GATHER * n_dev
    me = place[0]
    chip = me // 2

    def copies(k, dev, chunk, slot):
        row = dev * 2 * PER_GATHER + chunk
        return (pltpu.make_async_copy(toks[k].at[pl.ds(row * STAGE, STAGE)], xbuf.at[slot], sem.at[slot, 0]),
                pltpu.make_async_copy(toks[k].at[pl.ds((row + PER_GATHER) * STAGE, STAGE)], dybuf.at[slot], sem.at[slot, 1]))

    def fetch(i, slot):
        which = i // n_dev
        for k in range(n_arr):
            @pl.when(which // PER_GATHER == k)
            def _():
                for copy in copies(k, i - which * n_dev, which - k * PER_GATHER, slot):
                    copy.start()

    def put(ref, which):
        return pltpu.make_async_copy(outbuf, ref.at[:, pl.ds(which * STAGE, STAGE)], out_sem)

    fetch(0, 0)
    o1_ref[...] = jnp.zeros_like(o1_ref)
    o3_ref[...] = jnp.zeros_like(o3_ref)
    o2_ref[...] = jnp.zeros_like(o2_ref)

    def step(i, carry):
        slot = lax.rem(i, 2)
        which = i // n_dev
        dev = i - which * n_dev

        @pl.when(i + 1 < total)
        def _():
            fetch(i + 1, 1 - slot)
        for copy in copies(0, 0, 0, slot):
            copy.wait()
        x = xbuf[slot]
        dy = dybuf[slot]
        b1 = dot(x, w1_ref[...])
        b3 = dot(x, w3_ref[...])
        sig = jax.nn.sigmoid(b1)
        act = b1 * sig
        h = (act * b3).astype(BF16)
        hbuf[...] = h
        o2_ref[...] += dot_lt(h, dy)
        dh = dot_rt(dy, w2_ref[...])
        d1 = (dh * b3 * (sig * (1.0 + b1 * (1.0 - sig)))).astype(BF16)
        d1buf[...] = d1
        o1_ref[...] += dot_lt(x, d1)
        d3 = (dh * act).astype(BF16)
        d3buf[...] = d3
        o3_ref[...] += dot_lt(x, d3)

        @pl.when(dev // 2 == chip)
        def _():
            outbuf[0] = dot(hbuf[...], w2_ref[...])
            outbuf[1] = dot_rt(d1buf[...], w1_ref[...]) + dot_rt(d3buf[...], w3_ref[...])

            @pl.when(dev == me)
            def _():
                put(near_ref, which).start()

            @pl.when(dev != me)
            def _():
                put(far_ref, which).start()
            put(near_ref, 0).wait()
        return carry
    lax.fori_loop(0, total, step, 0)


def shared_half(toks, w1, w3, w2, me, n_dev):
    dim, width = w1.shape
    part = jax.ShapeDtypeStruct((2, CHUNKS * STAGE, dim), F32)
    small = pltpu.VMEM((STAGE, width), BF16)
    return pl.pallas_call(
        functools.partial(shared_kernel, len(toks), n_dev),
        out_shape=[jax.ShapeDtypeStruct((dim, width), F32), jax.ShapeDtypeStruct((dim, width), F32), jax.ShapeDtypeStruct((width, dim), F32), part, part],
        in_specs=[SMEM] + [HBM] * len(toks) + [VMEM] * 3,
        out_specs=[VMEM] * 3 + [HBM] * 2,
        scratch_shapes=[pltpu.VMEM((2, STAGE, dim), BF16), pltpu.VMEM((2, STAGE, dim), BF16), small, small, small,
                        pltpu.VMEM((2, STAGE, dim), F32), pltpu.SemaphoreType.DMA((2, 2)), pltpu.SemaphoreType.DMA],
        compiler_params=pltpu.CompilerParams(**PARAMS),
        cost_estimate=pl.CostEstimate(flops=170_000_000_000, bytes_accessed=160_000_000, transcendentals=0),
        name="shared_half",
    )(me[None], *toks, w1, w3, w2)


def finish_kernel(n_groups, sum_ref, near_ref, got_ref, *refs):
    y_ref, dx_ref = refs[-2:]

    def body(i, carry):
        rows16 = pl.ds(pl.multiple_of(i * 16, 16), 16)
        at = i * 16 * n_groups
        for which, out in ((0, y_ref), (1, dx_ref)):
            for c in range(n_groups):
                lanes = slice(c * LANE, (c + 1) * LANE)
                a = sum_ref[0, 0, which, pl.ds(at + c, SUB, stride=n_groups), :]
                b = sum_ref[0, 0, which, pl.ds(at + SUB * n_groups + c, SUB, stride=n_groups), :]
                val = jnp.concatenate([a, b], axis=0) + (near_ref[which, rows16, lanes] + got_ref[which, rows16, lanes])
                out[rows16, lanes] = val.astype(BF16)
        return carry
    lax.fori_loop(0, y_ref.shape[0] // 16, body, 0)


def finish(chunk, sums, where, near, got, held):
    n_tok, dim = near.shape[1:]
    n_groups = dim // LANE
    part = sums.shape[3] // n_groups
    row = pl.BlockSpec((part // 2, dim), lambda i: (2 * chunk + i, 0))
    both = pl.BlockSpec((2, part // 2, dim), lambda i: (0, 2 * chunk + i, 0))
    return pl.pallas_call(
        functools.partial(finish_kernel, n_groups),
        out_shape=[jax.ShapeDtypeStruct((n_tok, dim), BF16)] * 2,
        grid=(2,),
        in_specs=[pl.BlockSpec((1, 1, 2, sums.shape[3] // 2, LANE), lambda i: (0, where, 0, i, 0)), both, both] + [HBM] * len(held),
        out_specs=[row, row],
        input_output_aliases={3 + i: i for i in range(len(held))},
        compiler_params=pltpu.CompilerParams(dimension_semantics=("arbitrary",), **PARAMS),
        cost_estimate=pl.CostEstimate(flops=4_000_000_000, bytes_accessed=20_000_000, transcendentals=0),
        name="finish",
    )(sums, near, got, *held)


def route(ids_all, gates_all, first_expert, n_local, slot_cap):
    n_chunk, n_top, chunk_tok = ids_all.shape
    experts = first_expert + jnp.arange(n_local, dtype=jnp.int32)
    match = ids_all[:, None] == experts[None, :, None, None]
    hit = jnp.any(match, axis=2)
    gsel = jnp.sum(jnp.where(match, gates_all[:, None], 0.0), axis=2)
    n_seg = chunk_tok // LANE
    strict = (jnp.arange(LANE)[:, None] < jnp.arange(LANE)[None, :]).astype(BF16)
    seg = hit.reshape(n_chunk, n_local, n_seg, LANE)
    inner = jnp.einsum('cesl,lm->cesm', seg.astype(BF16), strict, preferred_element_type=F32)
    seg_sum = jnp.sum(seg, axis=3, dtype=jnp.int32)
    before = jnp.arange(n_seg)[:, None] < jnp.arange(n_seg)[None, :]
    outer = jnp.sum(jnp.where(before, seg_sum[..., :, None], 0), axis=2)
    rank = (inner.astype(jnp.int32) + outer[..., None]).reshape(n_chunk, n_local, chunk_tok)
    count = jnp.sum(seg_sum, axis=2)
    n_hi = slot_cap // 64
    hi = jnp.where(hit, rank >> 6, -1)
    lo = rank & 63
    pick_hi = (hi[:, :, None, :] == jnp.arange(n_hi, dtype=jnp.int32)[:, None]).astype(BF16)
    tok = jnp.arange(chunk_tok, dtype=jnp.int32)
    pick_lo = lo[:, :, None, :] == jnp.arange(64, dtype=jnp.int32)[:, None]
    val_lo = jnp.concatenate([jnp.where(pick_lo, (tok >> 6), 0), jnp.where(pick_lo, (tok & 63), 0)], axis=2).astype(BF16)
    found = jnp.einsum('ceht,cent->cehn', pick_hi, val_lo, preferred_element_type=F32).astype(jnp.int32)
    slots = (found[..., :64] * 64 + found[..., 64:]).reshape(n_chunk, n_local, slot_cap)
    slots = jnp.where(jnp.arange(slot_cap, dtype=jnp.int32) < count[..., None], slots, chunk_tok)
    n_blk = (count + BLK - 1) // BLK
    upto = jnp.cumsum(n_blk, axis=1)
    chunk_blk = upto[:, -1]
    chunk_off = jnp.cumsum(chunk_blk) - chunk_blk
    max_blk = n_local * (slot_cap // BLK)
    near = jnp.sum(seg_sum[..., :n_seg // 2], axis=2)
    at = jnp.arange(max_blk, dtype=jnp.int32)
    blk_e = jnp.minimum(jnp.sum(at[None, :, None] >= upto[:, None, :], axis=2, dtype=jnp.int32), n_local - 1)
    start = upto - n_blk
    of_blk = lambda v: jnp.sum(jnp.where(blk_e[..., None] == jnp.arange(n_local), v[:, None, :], 0), axis=2, dtype=jnp.int32)
    blk_k = at[None, :] - of_blk(start)
    blk_n = jnp.maximum(of_blk(count) - blk_k * BLK, 0)
    blk_near = jnp.maximum(of_blk(near) - blk_k * BLK, 0)
    glob = (chunk_off[:, None] + start).T.reshape(-1)
    cnt = n_blk.T.reshape(-1)
    end = jnp.cumsum(cnt)
    total_blk = end[-1]
    at2 = jnp.arange(n_local * slot_cap // BLK + n_chunk * n_local, dtype=jnp.int32)
    grp = jnp.minimum(jnp.sum(at2[:, None] >= end[None, :], axis=1, dtype=jnp.int32), cnt.shape[0] - 1)
    sel = grp[:, None] == jnp.arange(cnt.shape[0])
    order = at2 + jnp.sum(jnp.where(sel, (glob - (end - cnt))[None, :], 0), axis=1)
    order = jnp.clip(order, 0, at2.shape[0] - 1).astype(jnp.int32)
    owner = (grp // n_chunk).astype(jnp.int32)
    return slots, gsel, jnp.stack([blk_e, blk_k, blk_n, blk_near]).astype(jnp.int32), chunk_blk, chunk_off, order, owner, total_blk


def solution(mesh):
    ei_size = mesh.shape['ei']
    ex_size = mesh.shape['eo'] // 2
    n_chip = ei_size * ex_size
    group_size = 2 * n_chip
    split_mesh = jax.sharding.Mesh(mesh.devices.reshape(mesh.shape['dp'], ei_size, ex_size, 2), ('dp', 'ei', 'ex', 'core'))
    axes = ('ei', 'ex', 'core')
    chips = ('ei', 'ex')
    tok_spec = P(('dp', *axes), None)
    exp_spec = P(axes, None, None)
    full_spec = P(None, None)
    grad_spec = P(('dp', *axes), None, None)
    shared_spec = P('dp', None)

    def swap(v):
        return lax.ppermute(v, 'core', [(0, 1), (1, 0)])

    def device_step(x_loc, ids_loc, gates_loc, w_one, w_three, w_two, s_one, s_three, s_two, dy_loc):
        n_tok, n_top = ids_loc.shape
        dim = x_loc.shape[1]
        n_local = w_one.shape[0]
        n_exp = n_local * group_size
        cap = min(n_tok, CAP_FACTOR * ((n_tok * n_top + n_exp - 1) // n_exp))
        slot_cap = cap * group_size
        part = n_tok // CHUNKS
        chunk_tok = part * group_size
        core = lax.axis_index('core')
        me = (lax.axis_index('ei') * ex_size + lax.axis_index('ex')) * 2 + core

        span = PER_GATHER * part
        mine = [jnp.concatenate([v[k * span:(k + 1) * span] for v in (x_loc, dy_loc)]) for k in range(CHUNKS // PER_GATHER)]
        toks = [lax.all_gather(v, axes, axis=0, tiled=True) for v in lax.optimization_barrier(mine)]

        def near_first(v, axis):
            return jnp.where(core == 0, v, jnp.flip(v, axis))

        both = lax.all_gather(jnp.concatenate([ids_loc.T.astype(F32), gates_loc.T]), axes, axis=0)
        both = near_first(both.reshape(n_chip, 2, 2 * n_top, CHUNKS, part), 1).transpose(3, 2, 1, 0, 4).reshape(CHUNKS, 2 * n_top, chunk_tok)
        slots, gsel, blks, chunk_blk, chunk_off, order, owner, total_blk = route(
            both[:, :n_top].astype(jnp.int32), both[:, n_top:], me * n_local, n_local, slot_cap)
        n_rows = order.shape[0] * BLK

        held, saved = [], []
        sums, dg_parts = {}, []

        def finish_sums(c, x_rows):
            (group,) = [g for g in SCATTERS if c in g]
            where = group.index(c)
            total, dg_near = combine_rows(*rows, theirs, where, len(group), sums[group[where - 1]] if where else None)
            x_rows, total = lax.optimization_barrier((x_rows, total))
            sums[c] = total
            if c == group[-1]:
                total = lax.psum_scatter(total, chips, scatter_dimension=0, tiled=True)
                for k in group:
                    sums[k] = total
            dg_parts.append(jnp.concatenate([dg_near, dg_far])[:, :n_local].T.reshape(n_local, 2, n_chip, part))
            return x_rows

        for c in range(CHUNKS):
            meta = jnp.stack([chunk_blk[c], chunk_off[c], core]).astype(jnp.int32)
            gpad = jnp.concatenate([gsel[c].reshape(-1), jnp.zeros((LANE,), F32)])
            tables = (*blks[:, c], meta, slots[c].reshape(-1), gpad)
            x_rows, dy_rows, gate_rows = gather_rows(c % PER_GATHER, toks[c // PER_GATHER], held, (*tables[:3], *tables[4:]), n_rows, group_size)
            if c > 0:
                x_rows, theirs = lax.optimization_barrier((x_rows, theirs))
                x_rows = finish_sums(c - 1, x_rows)
            o_rows, dx_rows, dg, *saved = run_experts(x_rows, dy_rows, gate_rows, w_one, w_three, w_two, saved, tables[0], meta)
            rows = (o_rows, gate_rows, dg, dx_rows, tables, chunk_tok, n_chip)
            send, dg_far = combine_rows(*rows, None)
            theirs = swap(send)
            held = [x_rows, dy_rows, gate_rows]
        x_rows = finish_sums(CHUNKS - 1, x_rows)
        dw_one, dw_three, dw_two = weight_grads(x_rows, dy_rows, gate_rows, saved, order, owner, total_blk[None], n_local)

        width = s_one.shape[1] // 2
        toks, dw_one = lax.optimization_barrier((toks, dw_one))
        *halves, near, far = shared_half(toks, lax.dynamic_slice_in_dim(s_one, core * width, width, 1), lax.dynamic_slice_in_dim(s_three, core * width, width, 1),
                                         lax.dynamic_slice_in_dim(s_two, core * width, width, 0), me, group_size)
        got = swap(far)

        def join(mine, axis):
            theirs = swap(mine)
            return jnp.concatenate([jnp.where(core == 0, mine, theirs), jnp.where(core == 0, theirs, mine)], axis=axis)
        dws_one, dws_three, dws_two = join(halves[0], 1), join(halves[1], 1), join(halves[2], 0)

        dg_send = near_first(jnp.stack(dg_parts, axis=1), 2).transpose(3, 2, 0, 1, 4)
        dg_recv = lax.all_to_all(dg_send.reshape(group_size, n_local, n_tok), axes, 0, 0)
        dg_tok = dg_recv.reshape(n_exp, n_tok)
        pick = ids_loc.T[:, None, :] == jnp.arange(n_exp, dtype=jnp.int32)[:, None]
        d_gates = jnp.sum(jnp.where(pick, dg_tok[None], 0.0), axis=1).T

        outs = []
        for c in range(CHUNKS):
            outs = finish(c, sums[c], sum(g.index(c) for g in SCATTERS if c in g), near, got, outs)
        y_loc, dx_loc = outs
        return (y_loc, dx_loc, d_gates, dw_one, dw_three, dw_two, dws_one, dws_three, dws_two)

    return jax.shard_map(device_step, mesh=split_mesh, in_specs=(tok_spec, tok_spec, tok_spec, exp_spec, exp_spec, exp_spec, full_spec, full_spec, full_spec, tok_spec), out_specs=(tok_spec, tok_spec, tok_spec, grad_spec, grad_spec, grad_spec, shared_spec, shared_spec, shared_spec), check_vma=False)
```

```python
import functools

import jax
import jax.numpy as jnp
from jax import lax
from jax.experimental import pallas as pl
from jax.experimental.pallas import tpu as pltpu
from jax.sharding import PartitionSpec as P


CAP_FACTOR = 2
CHUNK_ROWS = (512, 768, 768)
CHUNKS = len(CHUNK_ROWS)
PITCH = max(CHUNK_ROWS)
STAGE = 256
BLK = 256
SHARED_ROWS = 512
LANE = 128
SUB = 8
F32 = jnp.float32
BF16 = jnp.bfloat16
SMEM = pl.BlockSpec(memory_space=pltpu.SMEM)
VMEM = pl.BlockSpec(memory_space=pltpu.VMEM)
HBM = pl.BlockSpec(memory_space=pl.ANY)
PARAMS = dict(vmem_limit_bytes=60 << 20)


def pipeline(body, n, in_specs=(), out_specs=()):
    return pltpu.emit_pipeline(lambda at, *refs: body(at.index[0], *refs), grid=(n,), in_specs=in_specs, out_specs=out_specs, _explicit_indices=True)


def dot(a, b):
    return jnp.dot(a, b, preferred_element_type=F32)


def dot_rt(a, b):
    return lax.dot_general(a, b, (((1,), (1,)), ((), ())), preferred_element_type=F32)


def dot_lt(a, b):
    return lax.dot_general(a, b, (((0,), (0,)), ((), ())), preferred_element_type=F32)


def lines_of(ref, row, n_groups):
    at = row * n_groups
    return ref[pl.ds(at, SUB), :], ref[pl.ds(at + SUB, n_groups - SUB), :]


def put_lines(ref, row, n_groups, val):
    at = row * n_groups
    ref[pl.ds(at, SUB), :] = val[0]
    ref[pl.ds(at + SUB, n_groups - SUB), :] = val[1]


def gather_kernel(part, chunk_tok, dim, slot_cap, n_dev, blk_e, blk_k, blk_n, meta, slots, gsel, tok_hbm, *refs):
    x_out, dy_out, g_out, stage, rowbuf = refs[-5:]
    n_groups = dim // LANE
    off = meta[1]
    core = meta[2]
    half = n_dev // 2
    steps = part // STAGE

    def clear(c, carry):
        stage[pl.ds(chunk_tok * n_groups + c, 1), :] = jnp.zeros((1, LANE), F32)
        return carry
    lax.fori_loop(0, n_groups, clear, 0)

    def fill(step, tok_ref):
        def convert(i, carry):
            at = ((step // steps) * PITCH + (step % steps) * STAGE + i * 16) * n_groups
            for c in range(n_groups):
                val = tok_ref[pl.ds(pl.multiple_of(i * 16, 16), 16), c * LANE:(c + 1) * LANE].astype(F32)
                stage[pl.ds(at + c, SUB, stride=n_groups), :] = val[:SUB]
                stage[pl.ds(at + SUB * n_groups + c, SUB, stride=n_groups), :] = val[SUB:]
            return carry
        lax.fori_loop(0, STAGE // 16, convert, 0)

    def rows(b, rows_ref, *gate):
        e = blk_e[b]
        base = e * slot_cap + blk_k[b] * BLK
        n_used = pl.cdiv(jnp.minimum(blk_n[b], BLK), 16)

        def move(g, carry):
            vals = []
            for r in range(16):
                t = slots[base + g * 16 + r]
                vals.append(lines_of(stage, t, n_groups))
                if gate:
                    gate[0][pl.ds(g * 16 + r, 1), :] = jnp.full((1, LANE), gsel[e * chunk_tok + t], F32)
            for r in range(16):
                put_lines(rowbuf, g * 16 + r, n_groups, vals[r])
            return carry
        lax.fori_loop(0, n_used, move, 0)

        def pack(i, carry):
            at = i * 16 * n_groups
            for c in range(n_groups):
                a = rowbuf[pl.ds(at + c, SUB, stride=n_groups), :]
                b2 = rowbuf[pl.ds(at + SUB * n_groups + c, SUB, stride=n_groups), :]
                rows_ref[pl.ds(pl.multiple_of(i * 16, 16), 16), c * LANE:(c + 1) * LANE] = jnp.concatenate([a, b2], axis=0).astype(BF16)
            return carry
        lax.fori_loop(0, n_used, pack, 0)

        def blank(i, carry):
            rows16 = pl.ds(pl.multiple_of(i * 16, 16), 16)
            rows_ref[rows16, :] = jnp.zeros((16, dim), BF16)
            if gate:
                gate[0][rows16, :] = jnp.zeros((16, LANE), F32)
            return carry
        lax.fori_loop(n_used, BLK // 16, blank, 0)

    row_spec = pl.BlockSpec((BLK, dim), lambda i: (off + i, 0))
    gate_spec = pl.BlockSpec((BLK, LANE), lambda i: (off + i, 0))

    def fill_all(which):
        far = lambda i: i // half
        dev = lambda i: 2 * (i - half * far(i)) + core + far(i) * (1 - 2 * core)
        row = lambda i: ((dev(i // steps) * 2 + which) * steps + i % steps, 0)
        pipeline(fill, n_dev * steps, in_specs=[pl.BlockSpec((STAGE, dim), row)])(tok_hbm)
    fill_all(0)
    pipeline(rows, meta[0], out_specs=[row_spec])(x_out)
    fill_all(1)
    pipeline(rows, meta[0], out_specs=[row_spec, gate_spec])(dy_out, g_out)


def gather_rows(tok, held, tables, n_rows, n_dev):
    dim = tok.shape[1]
    chunk_tok = PITCH * n_dev
    slot_cap = tables[4].shape[0] // 8
    return pl.pallas_call(
        functools.partial(gather_kernel, tok.shape[0] // (2 * n_dev), chunk_tok, dim, slot_cap, n_dev),
        out_shape=[jax.ShapeDtypeStruct((n_rows, dim), BF16), jax.ShapeDtypeStruct((n_rows, dim), BF16), jax.ShapeDtypeStruct((n_rows, LANE), F32)],
        in_specs=[SMEM] * 6 + [HBM] * (1 + len(held)),
        out_specs=[HBM] * 3,
        scratch_shapes=[pltpu.VMEM(((chunk_tok + 2) * dim // LANE, LANE), F32), pltpu.VMEM((BLK * dim // LANE, LANE), F32)],
        input_output_aliases={7 + i: i for i in range(len(held))},
        compiler_params=pltpu.CompilerParams(**PARAMS),
        cost_estimate=pl.CostEstimate(flops=30_000_000_000, bytes_accessed=120_000_000, transcendentals=0),
        name="gather_rows",
    )(*tables, tok, *held)


def scale_rows(gate, dy):
    return jnp.concatenate([(gate * dy[:, c * LANE:(c + 1) * LANE]).astype(BF16) for c in range(dy.shape[1] // LANE)], axis=1)


def expert_body(e, x_ref, dy_ref, g_ref, w1_ref, w3_ref, w2_ref, o_ref, dx_ref, dg_ref, h_ref, d1_ref, d3_ref):
    x = x_ref[...]
    a1 = dot(x, w1_ref[0])
    a3 = dot(x, w3_ref[0])
    sig = jax.nn.sigmoid(a1)
    act = a1 * sig
    h = (act * a3).astype(BF16)
    h_ref[...] = h
    o = dot(h, w2_ref[0]).astype(BF16)
    o_ref[...] = o
    dy = dy_ref[...].astype(F32)
    prod = dy * o.astype(F32)
    part = prod[:, 0:LANE]
    for c in range(1, prod.shape[1] // LANE):
        part = part + prod[:, c * LANE:(c + 1) * LANE]
    dg = jnp.sum(part, axis=1, keepdims=True)
    lane = lax.broadcasted_iota(jnp.int32, part.shape, 1)
    dg_ref[...] = jnp.where(lane == e, dg, 0.0)
    dh = dot_rt(scale_rows(g_ref[...], dy), w2_ref[0])
    d1 = (dh * a3 * (sig * (1.0 + a1 * (1.0 - sig)))).astype(BF16)
    d3 = (dh * act).astype(BF16)
    d1_ref[...] = d1
    d3_ref[...] = d3
    dx_ref[...] = (dot_rt(d1, w1_ref[0]) + dot_rt(d3, w3_ref[0])).astype(BF16)


def expert_kernel(blk_e, meta, x, dy, g, w1, w3, w2, *refs):
    outs = refs[-6:]
    dim, ffn = w1.shape[1:]
    off = meta[1]
    glob = lambda i: (off + i, 0)
    loc = lambda i: (i, 0)
    wmap = lambda i: (blk_e[i], 0, 0)
    pipeline(
        lambda b, *refs: expert_body(blk_e[b], *refs), meta[0],
        in_specs=[pl.BlockSpec((BLK, dim), glob), pl.BlockSpec((BLK, dim), glob), pl.BlockSpec((BLK, LANE), glob),
                  pl.BlockSpec((1, dim, ffn), wmap), pl.BlockSpec((1, dim, ffn), wmap), pl.BlockSpec((1, ffn, dim), wmap)],
        out_specs=[pl.BlockSpec((BLK, dim), loc), pl.BlockSpec((BLK, dim), loc), pl.BlockSpec((BLK, LANE), loc)]
        + [pl.BlockSpec((BLK, ffn), glob)] * 3)(x, dy, g, w1, w3, w2, *outs)


def run_experts(x_rows, dy_rows, gates, w1, w3, w2, saved, blk_e, meta):
    n_rows, dim = x_rows.shape
    loc_rows = blk_e.shape[0] * BLK
    return pl.pallas_call(
        expert_kernel,
        out_shape=[jax.ShapeDtypeStruct((loc_rows, dim), BF16), jax.ShapeDtypeStruct((loc_rows, dim), BF16),
                   jax.ShapeDtypeStruct((loc_rows, LANE), F32)] + [jax.ShapeDtypeStruct((n_rows, w1.shape[2]), BF16)] * 3,
        in_specs=[SMEM] * 2 + [HBM] * (6 + len(saved)),
        out_specs=[HBM] * 6,
        input_output_aliases={8 + i: 3 + i for i in range(len(saved))},
        compiler_params=pltpu.CompilerParams(**PARAMS),
        cost_estimate=pl.CostEstimate(flops=55_000_000_000, bytes_accessed=80_000_000, transcendentals=0),
        name="experts",
    )(blk_e, meta, x_rows, dy_rows, gates, w1, w3, w2, *saved)


def combine_kernel(far, n_groups, slot_cap, blk_e, blk_k, blk_n, blk_near, meta, slots, o_hbm, g_hbm, dg_hbm, dx_hbm, *refs):
    out_ref, dgo_ref, stage_y, stage_dx, stage_dg, rowbuf, sem = refs[-7:]
    n_chip = out_ref.shape[0]
    lines = out_ref.shape[2]
    half = n_chip * PITCH
    dim = n_groups * LANE
    off = meta[1]

    def rows(stage, b, rows_ref, *gate):
        base = blk_e[b] * slot_cap + blk_k[b] * BLK
        near = jnp.minimum(blk_near[b], BLK)
        if far:
            first, last = near, jnp.minimum(blk_n[b], BLK)
        else:
            first, last = 0, near

        def unpack(i, carry):
            at = i * 16 * n_groups
            rows16 = pl.ds(pl.multiple_of(i * 16, 16), 16)
            if gate:
                g16 = gate[0][rows16, :]
            for c in range(n_groups):
                val = rows_ref[rows16, c * LANE:(c + 1) * LANE].astype(F32)
                if gate:
                    val = val * g16
                rowbuf[pl.ds(at + c, SUB, stride=n_groups), :] = val[:SUB]
                rowbuf[pl.ds(at + SUB * n_groups + c, SUB, stride=n_groups), :] = val[SUB:]
            return carry
        lax.fori_loop(first // 16, pl.cdiv(last, 16), unpack, 0)

        def add(g, carry):
            todo = []
            for r in range(SUB):
                t = slots[base + g * SUB + r]
                if far:
                    t = t - half
                    t = jnp.where(t < 0, half, t)
                else:
                    t = jnp.minimum(t, half)
                a, b2 = lines_of(rowbuf, g * SUB + r, n_groups)
                old_a, old_b = lines_of(stage, t, n_groups)
                more = (stage_dg[pl.ds(t, 1), :] + gate[1][pl.ds(g * SUB + r, 1), :],) if gate else ()
                todo.append((t, (old_a + a, old_b + b2), more))
            for t, val, more in todo:
                put_lines(stage, t, n_groups, val)
                if gate:
                    stage_dg[pl.ds(t, 1), :] = more[0]
            return carry

        @pl.when(last > first)
        def _():
            lax.fori_loop(first // SUB, pl.cdiv(last, SUB), add, 0)

    def clear(stage, n):
        def zero(i, carry):
            for k in range(8):
                stage[pl.ds(pl.multiple_of(i * 64 + k * SUB, SUB), SUB), :] = jnp.zeros((SUB, LANE), F32)
            return carry
        lax.fori_loop(0, n // 64, zero, 0)

    def loads(stage, which):
        return [pltpu.make_async_copy(refs[0].at[j, which], stage.at[pl.ds(j * PITCH * n_groups, lines)], sem.at[3 + which]) for j in range(n_chip)]

    def stores(stage, which):
        return [pltpu.make_async_copy(stage.at[pl.ds(j * PITCH * n_groups, lines)], out_ref.at[j, which], sem.at[which]) for j in range(n_chip)]

    def start(copies):
        for copy in copies:
            copy.start()

    def wait(copies):
        for copy in copies:
            copy.wait()

    row_spec = pl.BlockSpec((BLK, dim), lambda i: (i, 0))
    if not far:
        start(loads(stage_y, 0))
        start(loads(stage_dx, 1))
    clear(stage_dg, half)
    if far:
        clear(stage_y, half * n_groups)
    else:
        wait(loads(stage_y, 0))
    pipeline(functools.partial(rows, stage_y), meta[0],
             in_specs=[row_spec, pl.BlockSpec((BLK, LANE), lambda i: (off + i, 0)), pl.BlockSpec((BLK, LANE), lambda i: (i, 0))])(o_hbm, g_hbm, dg_hbm)
    out = stores(stage_y, 0) + [pltpu.make_async_copy(stage_dg.at[pl.ds(0, half)], dgo_ref, sem.at[2])]
    start(out)
    if far:
        clear(stage_dx, half * n_groups)
    else:
        wait(loads(stage_dx, 1))
    pipeline(functools.partial(rows, stage_dx), meta[0], in_specs=[row_spec])(dx_hbm)
    start(stores(stage_dx, 1))
    wait(out + stores(stage_dx, 1))


def combine_rows(o_rows, gates, dg, dx_rows, tables, part, n_chip, theirs):
    n_groups = o_rows.shape[1] // LANE
    blk_e, blk_k, blk_n, blk_near, meta, slots, _ = tables
    half = n_chip * PITCH
    more = [] if theirs is None else [theirs]
    stage = pltpu.VMEM(((half + 2) * n_groups, LANE), F32)
    return pl.pallas_call(
        functools.partial(combine_kernel, theirs is None, n_groups, slots.shape[0] // 8),
        out_shape=[jax.ShapeDtypeStruct((n_chip, 2, part * n_groups, LANE), F32), jax.ShapeDtypeStruct((half, LANE), F32)],
        in_specs=[SMEM] * 6 + [HBM] * (4 + len(more)),
        out_specs=[HBM] * 2,
        scratch_shapes=[stage, stage, pltpu.VMEM((half + SUB, LANE), F32), pltpu.VMEM((BLK * n_groups, LANE), F32), pltpu.SemaphoreType.DMA((5,))],
        compiler_params=pltpu.CompilerParams(**PARAMS),
        cost_estimate=pl.CostEstimate(flops=20_000_000_000, bytes_accessed=60_000_000, transcendentals=0),
        name="combine_far" if theirs is None else "combine_near",
    )(blk_e, blk_k, blk_n, blk_near, meta, slots, o_rows, gates, dg, dx_rows, *more)


def grad_kernel(order, owner, total, x, dy, g, h, d1, d3, o1, o3, o2, acc1, acc3, acc2):
    dim, ffn = o1.shape[1:]
    n = total[0]

    def step(i, x_ref, dy_ref, g_ref, h_ref, d1_ref, d3_ref, o1_ref, o3_ref, o2_ref):
        e = owner[i]
        first = jnp.logical_or(i == 0, owner[jnp.maximum(i - 1, 0)] != e)
        last = jnp.logical_or(i == n - 1, owner[jnp.minimum(i + 1, owner.shape[0] - 1)] != e)

        @pl.when(first)
        def _():
            acc1[...] = jnp.zeros_like(acc1)
            acc3[...] = jnp.zeros_like(acc3)
            acc2[...] = jnp.zeros_like(acc2)

        x = x_ref[...]
        acc1[...] += dot_lt(x, d1_ref[...])
        acc3[...] += dot_lt(x, d3_ref[...])
        acc2[...] += dot_lt(h_ref[...], scale_rows(g_ref[...], dy_ref[...].astype(F32)))

        @pl.when(last)
        def _():
            o1_ref[0] = acc1[...].astype(BF16)
            o3_ref[0] = acc3[...].astype(BF16)
            o2_ref[0] = acc2[...].astype(BF16)
    row = lambda i: (order[i], 0)
    wmap = lambda i: (owner[i], 0, 0)
    pipeline(
        step, n,
        in_specs=[pl.BlockSpec((BLK, dim), row), pl.BlockSpec((BLK, dim), row), pl.BlockSpec((BLK, LANE), row)]
        + [pl.BlockSpec((BLK, ffn), row)] * 3,
        out_specs=[pl.BlockSpec((1, dim, ffn), wmap), pl.BlockSpec((1, dim, ffn), wmap), pl.BlockSpec((1, ffn, dim), wmap)],
    )(x, dy, g, h, d1, d3, o1, o3, o2)


def weight_grads(x_rows, dy_rows, gates, saved, order, owner, total, n_local):
    dim = x_rows.shape[1]
    ffn = saved[0].shape[1]
    return pl.pallas_call(
        grad_kernel,
        out_shape=[jax.ShapeDtypeStruct((n_local, dim, ffn), BF16), jax.ShapeDtypeStruct((n_local, dim, ffn), BF16),
                   jax.ShapeDtypeStruct((n_local, ffn, dim), BF16)],
        in_specs=[SMEM] * 3 + [HBM] * 6,
        out_specs=[HBM] * 3,
        scratch_shapes=[pltpu.VMEM((dim, ffn), F32), pltpu.VMEM((dim, ffn), F32), pltpu.VMEM((ffn, dim), F32)],
        compiler_params=pltpu.CompilerParams(**PARAMS),
        cost_estimate=pl.CostEstimate(flops=100_000_000_000, bytes_accessed=160_000_000, transcendentals=0),
        name="weight_grads",
    )(order, owner, total, x_rows, dy_rows, gates, *saved)


def shared_kernel(n_arr, n_dev, place, *refs):
    toks = refs[:n_arr]
    w1_ref, w3_ref, w2_ref, o1_ref, o3_ref, o2_ref, near_ref, far_ref, xbuf, dybuf, hbuf, d1buf, d3buf, outbuf, sem, out_sem = refs[n_arr:]
    me = place[0]
    chip = me // 2
    pieces = [(k, r) for k, rows in enumerate(CHUNK_ROWS) for r in range(0, rows, STAGE)]
    per_step = SHARED_ROWS // STAGE
    steps = len(pieces) // per_step
    total = n_dev * steps

    def copies(dev, s, slot):
        made = []
        for p in range(per_step):
            k, r = pieces[s * per_step + p]
            row = dev * 2 * CHUNK_ROWS[k] + r
            to = pl.ds(p * STAGE, STAGE)
            made.append(pltpu.make_async_copy(toks[k].at[pl.ds(row, STAGE)], xbuf.at[slot, to], sem.at[slot, 0]))
            made.append(pltpu.make_async_copy(toks[k].at[pl.ds(row + CHUNK_ROWS[k], STAGE)], dybuf.at[slot, to], sem.at[slot, 1]))
        return made

    def fetch(i, slot):
        for s in range(steps):
            @pl.when(i % steps == s)
            def _():
                for copy in copies(i // steps, s, slot):
                    copy.start()

    def put(ref, which):
        return pltpu.make_async_copy(outbuf, ref.at[:, pl.ds(which * SHARED_ROWS, SHARED_ROWS)], out_sem)

    fetch(0, 0)
    o1_ref[...] = jnp.zeros_like(o1_ref)
    o3_ref[...] = jnp.zeros_like(o3_ref)
    o2_ref[...] = jnp.zeros_like(o2_ref)

    def step(i, carry):
        slot = lax.rem(i, 2)
        dev = i // steps
        which = i - dev * steps

        @pl.when(i + 1 < total)
        def _():
            fetch(i + 1, 1 - slot)
        for copy in copies(0, 0, slot):
            copy.wait()
        x = xbuf[slot]
        dy = dybuf[slot]
        b1 = dot(x, w1_ref[...])
        b3 = dot(x, w3_ref[...])
        sig = jax.nn.sigmoid(b1)
        act = b1 * sig
        h = (act * b3).astype(BF16)
        hbuf[...] = h
        o2_ref[...] += dot_lt(h, dy)
        dh = dot_rt(dy, w2_ref[...])
        d1 = (dh * b3 * (sig * (1.0 + b1 * (1.0 - sig)))).astype(BF16)
        d1buf[...] = d1
        o1_ref[...] += dot_lt(x, d1)
        d3 = (dh * act).astype(BF16)
        d3buf[...] = d3
        o3_ref[...] += dot_lt(x, d3)

        @pl.when(dev // 2 == chip)
        def _():
            outbuf[0] = dot(hbuf[...], w2_ref[...])
            outbuf[1] = dot_rt(d1buf[...], w1_ref[...]) + dot_rt(d3buf[...], w3_ref[...])

            @pl.when(dev == me)
            def _():
                put(near_ref, which).start()

            @pl.when(dev != me)
            def _():
                put(far_ref, which).start()
            put(near_ref, 0).wait()
        return carry
    lax.fori_loop(0, total, step, 0)


def shared_half(toks, w1, w3, w2, me, n_dev):
    dim, width = w1.shape
    part = jax.ShapeDtypeStruct((2, sum(CHUNK_ROWS), dim), F32)
    small = pltpu.VMEM((SHARED_ROWS, width), BF16)
    return pl.pallas_call(
        functools.partial(shared_kernel, len(toks), n_dev),
        out_shape=[jax.ShapeDtypeStruct((dim, width), F32), jax.ShapeDtypeStruct((dim, width), F32), jax.ShapeDtypeStruct((width, dim), F32), part, part],
        in_specs=[SMEM] + [HBM] * len(toks) + [VMEM] * 3,
        out_specs=[VMEM] * 3 + [HBM] * 2,
        scratch_shapes=[pltpu.VMEM((2, SHARED_ROWS, dim), BF16), pltpu.VMEM((2, SHARED_ROWS, dim), BF16), small, small, small,
                        pltpu.VMEM((2, SHARED_ROWS, dim), F32), pltpu.SemaphoreType.DMA((2, 2)), pltpu.SemaphoreType.DMA],
        compiler_params=pltpu.CompilerParams(**PARAMS),
        cost_estimate=pl.CostEstimate(flops=170_000_000_000, bytes_accessed=160_000_000, transcendentals=0),
        name="shared_half",
    )(me[None], *toks, w1, w3, w2)


def finish_kernel(n_groups, sum_ref, near_ref, got_ref, *refs):
    y_ref, dx_ref = refs[-2:]

    def body(i, carry):
        rows16 = pl.ds(pl.multiple_of(i * 16, 16), 16)
        at = i * 16 * n_groups
        for which, out in ((0, y_ref), (1, dx_ref)):
            for c in range(n_groups):
                lanes = slice(c * LANE, (c + 1) * LANE)
                a = sum_ref[0, which, pl.ds(at + c, SUB, stride=n_groups), :]
                b = sum_ref[0, which, pl.ds(at + SUB * n_groups + c, SUB, stride=n_groups), :]
                val = jnp.concatenate([a, b], axis=0) + (near_ref[which, rows16, lanes] + got_ref[which, rows16, lanes])
                out[rows16, lanes] = val.astype(BF16)
        return carry
    lax.fori_loop(0, y_ref.shape[0] // 16, body, 0)


def finish(chunk, sums, near, got, held):
    n_tok, dim = near.shape[1:]
    n_groups = dim // LANE
    first = sum(CHUNK_ROWS[:chunk]) // STAGE
    row = pl.BlockSpec((STAGE, dim), lambda i: (first + i, 0))
    both = pl.BlockSpec((2, STAGE, dim), lambda i: (0, first + i, 0))
    return pl.pallas_call(
        functools.partial(finish_kernel, n_groups),
        out_shape=[jax.ShapeDtypeStruct((n_tok, dim), BF16)] * 2,
        grid=(CHUNK_ROWS[chunk] // STAGE,),
        in_specs=[pl.BlockSpec((1, 2, STAGE * n_groups, LANE), lambda i: (0, 0, i, 0)), both, both] + [HBM] * len(held),
        out_specs=[row, row],
        input_output_aliases={3 + i: i for i in range(len(held))},
        compiler_params=pltpu.CompilerParams(dimension_semantics=("arbitrary",), **PARAMS),
        cost_estimate=pl.CostEstimate(flops=4_000_000_000, bytes_accessed=20_000_000, transcendentals=0),
        name="finish",
    )(sums, near, got, *held)


def route(ids_all, gates_all, first_expert, n_local, slot_cap):
    n_chunk, n_top, chunk_tok = ids_all.shape
    experts = first_expert + jnp.arange(n_local, dtype=jnp.int32)
    match = ids_all[:, None] == experts[None, :, None, None]
    hit = jnp.any(match, axis=2)
    gsel = jnp.sum(jnp.where(match, gates_all[:, None], 0.0), axis=2)
    n_seg = chunk_tok // LANE
    strict = (jnp.arange(LANE)[:, None] < jnp.arange(LANE)[None, :]).astype(BF16)
    seg = hit.reshape(n_chunk, n_local, n_seg, LANE)
    inner = jnp.einsum('cesl,lm->cesm', seg.astype(BF16), strict, preferred_element_type=F32)
    seg_sum = jnp.sum(seg, axis=3, dtype=jnp.int32)
    before = jnp.arange(n_seg)[:, None] < jnp.arange(n_seg)[None, :]
    outer = jnp.sum(jnp.where(before, seg_sum[..., :, None], 0), axis=2)
    rank = (inner.astype(jnp.int32) + outer[..., None]).reshape(n_chunk, n_local, chunk_tok)
    count = jnp.sum(seg_sum, axis=2)
    n_hi = slot_cap // 64
    hi = jnp.where(hit, rank >> 6, -1)
    lo = rank & 63
    pick_hi = (hi[:, :, None, :] == jnp.arange(n_hi, dtype=jnp.int32)[:, None]).astype(BF16)
    tok = jnp.arange(chunk_tok, dtype=jnp.int32)
    pick_lo = lo[:, :, None, :] == jnp.arange(64, dtype=jnp.int32)[:, None]
    val_lo = jnp.concatenate([jnp.where(pick_lo, (tok >> 6), 0), jnp.where(pick_lo, (tok & 63), 0)], axis=2).astype(BF16)
    found = jnp.einsum('ceht,cent->cehn', pick_hi, val_lo, preferred_element_type=F32).astype(jnp.int32)
    slots = (found[..., :64] * 64 + found[..., 64:]).reshape(n_chunk, n_local, slot_cap)
    slots = jnp.where(jnp.arange(slot_cap, dtype=jnp.int32) < count[..., None], slots, chunk_tok)
    n_blk = (count + BLK - 1) // BLK
    upto = jnp.cumsum(n_blk, axis=1)
    chunk_blk = upto[:, -1]
    chunk_off = jnp.cumsum(chunk_blk) - chunk_blk
    max_blk = n_local * (slot_cap // BLK)
    near = jnp.sum(seg_sum[..., :n_seg // 2], axis=2)
    at = jnp.arange(max_blk, dtype=jnp.int32)
    blk_e = jnp.minimum(jnp.sum(at[None, :, None] >= upto[:, None, :], axis=2, dtype=jnp.int32), n_local - 1)
    start = upto - n_blk
    of_blk = lambda v: jnp.sum(jnp.where(blk_e[..., None] == jnp.arange(n_local), v[:, None, :], 0), axis=2, dtype=jnp.int32)
    blk_k = at[None, :] - of_blk(start)
    blk_n = jnp.maximum(of_blk(count) - blk_k * BLK, 0)
    blk_near = jnp.maximum(of_blk(near) - blk_k * BLK, 0)
    glob = (chunk_off[:, None] + start).T.reshape(-1)
    cnt = n_blk.T.reshape(-1)
    end = jnp.cumsum(cnt)
    total_blk = end[-1]
    at2 = jnp.arange(n_local * slot_cap // BLK + n_chunk * n_local, dtype=jnp.int32)
    grp = jnp.minimum(jnp.sum(at2[:, None] >= end[None, :], axis=1, dtype=jnp.int32), cnt.shape[0] - 1)
    sel = grp[:, None] == jnp.arange(cnt.shape[0])
    order = at2 + jnp.sum(jnp.where(sel, (glob - (end - cnt))[None, :], 0), axis=1)
    order = jnp.clip(order, 0, at2.shape[0] - 1).astype(jnp.int32)
    owner = (grp // n_chunk).astype(jnp.int32)
    return slots, gsel, jnp.stack([blk_e, blk_k, blk_n, blk_near]).astype(jnp.int32), chunk_blk, chunk_off, order, owner, total_blk


def solution(mesh):
    ei_size = mesh.shape['ei']
    ex_size = mesh.shape['eo'] // 2
    n_chip = ei_size * ex_size
    group_size = 2 * n_chip
    split_mesh = jax.sharding.Mesh(mesh.devices.reshape(mesh.shape['dp'], ei_size, ex_size, 2), ('dp', 'ei', 'ex', 'core'))
    axes = ('ei', 'ex', 'core')
    chips = ('ei', 'ex')
    tok_spec = P(('dp', *axes), None)
    exp_spec = P(axes, None, None)
    full_spec = P(None, None)
    grad_spec = P(('dp', *axes), None, None)
    shared_spec = P('dp', None)

    def swap(v):
        return lax.ppermute(v, 'core', [(0, 1), (1, 0)])

    def device_step(x_loc, ids_loc, gates_loc, w_one, w_three, w_two, s_one, s_three, s_two, dy_loc):
        n_tok, n_top = ids_loc.shape
        dim = x_loc.shape[1]
        n_local = w_one.shape[0]
        n_exp = n_local * group_size
        cap = min(n_tok, CAP_FACTOR * ((n_tok * n_top + n_exp - 1) // n_exp))
        slot_cap = cap * group_size
        chunk_tok = PITCH * group_size
        rows_of = [slice(sum(CHUNK_ROWS[:c]), sum(CHUNK_ROWS[:c + 1])) for c in range(CHUNKS)]
        core = lax.axis_index('core')
        me = (lax.axis_index('ei') * ex_size + lax.axis_index('ex')) * 2 + core

        mine = [jnp.concatenate([x_loc[r], dy_loc[r]]) for r in rows_of]
        toks = [lax.all_gather(v, axes, axis=0, tiled=True) for v in lax.optimization_barrier(mine)]

        def near_first(v, axis):
            return jnp.where(core == 0, v, jnp.flip(v, axis))

        both = jnp.concatenate([ids_loc.T.astype(F32), gates_loc.T])
        both = jnp.stack([jnp.pad(both[:, r], ((0, 0), (0, PITCH - (r.stop - r.start))), constant_values=-1.0) for r in rows_of])
        both = near_first(lax.all_gather(both, axes, axis=0).reshape(n_chip, 2, CHUNKS, 2 * n_top, PITCH), 1)
        both = both.transpose(2, 3, 1, 0, 4).reshape(CHUNKS, 2 * n_top, chunk_tok)
        slots, gsel, blks, chunk_blk, chunk_off, order, owner, total_blk = route(
            both[:, :n_top].astype(jnp.int32), both[:, n_top:], me * n_local, n_local, slot_cap)
        n_rows = order.shape[0] * BLK

        held, saved = [], []
        sums, dg_parts = [], []

        def finish_sums(c, x_rows, gate_rows):
            total, dg_near = combine_rows(o_rows, gate_rows, dg, dx_rows, tables, CHUNK_ROWS[c], n_chip, theirs)
            x_rows, total = lax.optimization_barrier((x_rows, total))
            sums.append(lax.psum_scatter(total, chips, scatter_dimension=0, tiled=True))
            dg_parts.append(jnp.concatenate([dg_near, dg_far])[:, :n_local].T.reshape(n_local, 2, n_chip, PITCH)[..., :CHUNK_ROWS[c]])
            return x_rows

        for c in range(CHUNKS):
            meta = jnp.stack([chunk_blk[c], chunk_off[c], core]).astype(jnp.int32)
            gpad = jnp.concatenate([gsel[c].reshape(-1), jnp.zeros((LANE,), F32)])
            now = (*blks[:, c], meta, slots[c].reshape(-1), gpad)
            x_rows, dy_rows, gate_rows = gather_rows(toks[c], held, (*now[:3], *now[4:]), n_rows, group_size)
            if c > 0:
                x_rows, theirs = lax.optimization_barrier((x_rows, theirs))
                x_rows = finish_sums(c - 1, x_rows, gate_rows)
            tables = now
            o_rows, dx_rows, dg, *saved = run_experts(x_rows, dy_rows, gate_rows, w_one, w_three, w_two, saved, tables[0], meta)
            send, dg_far = combine_rows(o_rows, gate_rows, dg, dx_rows, tables, CHUNK_ROWS[c], n_chip, None)
            theirs = swap(send)
            held = [x_rows, dy_rows, gate_rows]
        x_rows = finish_sums(CHUNKS - 1, x_rows, gate_rows)
        dw_one, dw_three, dw_two = weight_grads(x_rows, dy_rows, gate_rows, saved, order, owner, total_blk[None], n_local)

        width = s_one.shape[1] // 2
        toks, dw_one = lax.optimization_barrier((toks, dw_one))
        *halves, near, far = shared_half(toks, lax.dynamic_slice_in_dim(s_one, core * width, width, 1), lax.dynamic_slice_in_dim(s_three, core * width, width, 1),
                                         lax.dynamic_slice_in_dim(s_two, core * width, width, 0), me, group_size)
        got = swap(far)

        def join(mine, axis):
            theirs = swap(mine)
            return jnp.concatenate([jnp.where(core == 0, mine, theirs), jnp.where(core == 0, theirs, mine)], axis=axis)
        dws_one, dws_three, dws_two = join(halves[0], 1), join(halves[1], 1), join(halves[2], 0)

        dg_send = near_first(jnp.concatenate(dg_parts, axis=3), 1).transpose(2, 1, 0, 3)
        dg_recv = lax.all_to_all(dg_send.reshape(group_size, n_local, n_tok), axes, 0, 0)
        dg_tok = dg_recv.reshape(n_exp, n_tok)
        pick = ids_loc.T[:, None, :] == jnp.arange(n_exp, dtype=jnp.int32)[:, None]
        d_gates = jnp.sum(jnp.where(pick, dg_tok[None], 0.0), axis=1).T

        outs = []
        for c in range(CHUNKS):
            outs = finish(c, sums[c], near, got, outs)
        y_loc, dx_loc = outs
        return (y_loc, dx_loc, d_gates, dw_one, dw_three, dw_two, dws_one, dws_three, dws_two)

    return jax.shard_map(device_step, mesh=split_mesh, in_specs=(tok_spec, tok_spec, tok_spec, exp_spec, exp_spec, exp_spec, full_spec, full_spec, full_spec, tok_spec), out_specs=(tok_spec, tok_spec, tok_spec, grad_spec, grad_spec, grad_spec, shared_spec, shared_spec, shared_spec), check_vma=False)
```

```python
import functools

import jax
import jax.numpy as jnp
from jax import lax
from jax.experimental import pallas as pl
from jax.experimental.pallas import tpu as pltpu
from jax.sharding import PartitionSpec as P


CAP_FACTOR = 2
CHUNKS = 4
PER_GATHER = 2
SCATTERS = ((0,), (1, 2), (3,))
BLK = 256
STAGE = 512
LANE = 128
SUB = 8
F32 = jnp.float32
BF16 = jnp.bfloat16
SMEM = pl.BlockSpec(memory_space=pltpu.SMEM)
VMEM = pl.BlockSpec(memory_space=pltpu.VMEM)
HBM = pl.BlockSpec(memory_space=pl.ANY)
PARAMS = dict(vmem_limit_bytes=60 << 20)


def pipeline(body, n, in_specs=(), out_specs=()):
    return pltpu.emit_pipeline(lambda at, *refs: body(at.index[0], *refs), grid=(n,), in_specs=in_specs, out_specs=out_specs, _explicit_indices=True)


def dot(a, b):
    return jnp.dot(a, b, preferred_element_type=F32)


def dot_rt(a, b):
    return lax.dot_general(a, b, (((1,), (1,)), ((), ())), preferred_element_type=F32)


def dot_lt(a, b):
    return lax.dot_general(a, b, (((0,), (0,)), ((), ())), preferred_element_type=F32)


def lines_of(ref, row, n_groups):
    at = row * n_groups
    return ref[pl.ds(at, SUB), :], ref[pl.ds(at + SUB, n_groups - SUB), :]


def put_lines(ref, row, n_groups, val):
    at = row * n_groups
    ref[pl.ds(at, SUB), :] = val[0]
    ref[pl.ds(at + SUB, n_groups - SUB), :] = val[1]


def rows_to_lines(lines_ref, first, val, c, n_groups):
    at = first * n_groups + c
    lines_ref[pl.ds(at, SUB, stride=n_groups), :] = val[:SUB]
    lines_ref[pl.ds(at + SUB * n_groups, SUB, stride=n_groups), :] = val[SUB:]


def lines_to_rows(lines_ref, first, c, n_groups):
    at = first * n_groups + c
    return jnp.concatenate([lines_ref[pl.ds(at, SUB, stride=n_groups), :], lines_ref[pl.ds(at + SUB * n_groups, SUB, stride=n_groups), :]], axis=0)


def clear_lines(ref, n):
    def zero(i, carry):
        for k in range(32):
            ref[pl.ds(pl.multiple_of(i * 256 + k * SUB, SUB), SUB), :] = jnp.zeros((SUB, LANE), F32)
        return carry
    lax.fori_loop(0, n // 256, zero, 0)


def sixteen(i):
    return pl.ds(pl.multiple_of(i * 16, 16), 16)


def gather_kernel(chunk, chunk_tok, dim, slot_cap, blk_e, blk_k, blk_n, meta, slots, gsel, tok_hbm, *refs):
    x_out, dy_out, g_out, stage_x, stage_dy, buf_x, buf_dy = refs[-7:]
    n_groups = dim // LANE
    off = meta[1]

    def clear(c, carry):
        for stage in (stage_x, stage_dy):
            stage[pl.ds(chunk_tok * n_groups + c, 1), :] = jnp.zeros((1, LANE), F32)
        return carry
    lax.fori_loop(0, n_groups, clear, 0)

    def fill(step, x_ref, dy_ref):
        def convert(i, carry):
            for ref, stage in ((x_ref, stage_x), (dy_ref, stage_dy)):
                for c in range(n_groups):
                    rows_to_lines(stage, step * STAGE + i * 16, ref[sixteen(i), c * LANE:(c + 1) * LANE].astype(F32), c, n_groups)
            return carry
        lax.fori_loop(0, STAGE // 16, convert, 0)

    def rows(b, x_ref, dy_ref, g_ref):
        e = blk_e[b]
        base = e * slot_cap + blk_k[b] * BLK
        n_used = pl.cdiv(jnp.minimum(blk_n[b], BLK), 16)

        def move(g, carry):
            vals = []
            for r in range(SUB):
                t = slots[base + g * SUB + r]
                vals.append((lines_of(stage_x, t, n_groups), lines_of(stage_dy, t, n_groups)))
                g_ref[pl.ds(g * SUB + r, 1), :] = jnp.full((1, LANE), gsel[e * chunk_tok + t], F32)
            for r in range(SUB):
                put_lines(buf_x, g * SUB + r, n_groups, vals[r][0])
                put_lines(buf_dy, g * SUB + r, n_groups, vals[r][1])
            return carry
        lax.fori_loop(0, 2 * n_used, move, 0)

        def pack(i, carry):
            for c in range(n_groups):
                for buf, ref in ((buf_x, x_ref), (buf_dy, dy_ref)):
                    ref[sixteen(i), c * LANE:(c + 1) * LANE] = lines_to_rows(buf, i * 16, c, n_groups).astype(BF16)
            return carry
        lax.fori_loop(0, n_used, pack, 0)

        def blank(i, carry):
            x_ref[sixteen(i), :] = jnp.zeros((16, dim), BF16)
            dy_ref[sixteen(i), :] = jnp.zeros((16, dim), BF16)
            g_ref[sixteen(i), :] = jnp.zeros((16, LANE), F32)
            return carry
        lax.fori_loop(n_used, BLK // 16, blank, 0)

    spec = lambda which: pl.BlockSpec((STAGE, dim), lambda i: ((i * 2 + which) * PER_GATHER + chunk, 0))
    pipeline(fill, chunk_tok // STAGE, in_specs=[spec(0), spec(1)])(tok_hbm, tok_hbm)
    out = lambda width: pl.BlockSpec((BLK, width), lambda i: (off + i, 0))
    pipeline(rows, meta[0], out_specs=[out(dim), out(dim), out(LANE)])(x_out, dy_out, g_out)


def gather_rows(chunk, tok, held, tables, n_rows, n_chip):
    dim = tok.shape[1]
    chunk_tok = STAGE * n_chip
    blk_e, blk_k, blk_n, meta, slots, gsel, n_exp = tables
    stage = pltpu.VMEM(((chunk_tok + 2) * dim // LANE, LANE), F32)
    buf = pltpu.VMEM((BLK * dim // LANE, LANE), F32)
    return pl.pallas_call(
        functools.partial(gather_kernel, chunk, chunk_tok, dim, slots.shape[0] // n_exp),
        out_shape=[jax.ShapeDtypeStruct((n_rows, dim), BF16), jax.ShapeDtypeStruct((n_rows, dim), BF16), jax.ShapeDtypeStruct((n_rows, LANE), F32)],
        in_specs=[SMEM] * 6 + [HBM] * (1 + len(held)),
        out_specs=[HBM] * 3,
        scratch_shapes=[stage, stage, buf, buf],
        input_output_aliases={7 + i: i for i in range(len(held))},
        compiler_params=pltpu.CompilerParams(**PARAMS),
        cost_estimate=pl.CostEstimate(flops=30_000_000_000, bytes_accessed=120_000_000, transcendentals=0),
        name="gather_rows",
    )(blk_e, blk_k, blk_n, meta, slots, gsel, tok, *held)


def scale_rows(gate, dy):
    return jnp.concatenate([(gate * dy[:, c * LANE:(c + 1) * LANE]).astype(BF16) for c in range(dy.shape[1] // LANE)], axis=1)


def expert_body(e, x_ref, dy_ref, g_ref, w1_ref, w3_ref, w2_ref, o_ref, dx_ref, dg_ref, h_ref, d1_ref, d3_ref):
    x = x_ref[...]
    a1 = dot(x, w1_ref[0])
    a3 = dot(x, w3_ref[0])
    sig = jax.nn.sigmoid(a1)
    act = a1 * sig
    h = (act * a3).astype(BF16)
    h_ref[...] = h
    o = dot(h, w2_ref[0]).astype(BF16)
    o_ref[...] = o
    dy = dy_ref[...].astype(F32)
    prod = dy * o.astype(F32)
    part = prod[:, 0:LANE]
    for c in range(1, prod.shape[1] // LANE):
        part = part + prod[:, c * LANE:(c + 1) * LANE]
    dg = jnp.sum(part, axis=1, keepdims=True)
    lane = lax.broadcasted_iota(jnp.int32, part.shape, 1)
    dg_ref[...] = jnp.where(lane == e, dg, 0.0)
    dh = dot_rt(scale_rows(g_ref[...], dy), w2_ref[0])
    d1 = (dh * a3 * (sig * (1.0 + a1 * (1.0 - sig)))).astype(BF16)
    d3 = (dh * act).astype(BF16)
    d1_ref[...] = d1
    d3_ref[...] = d3
    dx_ref[...] = (dot_rt(d1, w1_ref[0]) + dot_rt(d3, w3_ref[0])).astype(BF16)


def expert_kernel(blk_e, meta, x, dy, g, w1, w3, w2, *refs):
    outs = refs[-6:]
    dim, ffn = w1.shape[1:]
    off = meta[1]
    glob = lambda i: (off + i, 0)
    loc = lambda i: (i, 0)
    wmap = lambda i: (blk_e[i], 0, 0)
    pipeline(
        lambda b, *refs: expert_body(blk_e[b], *refs), meta[0],
        in_specs=[pl.BlockSpec((BLK, dim), glob), pl.BlockSpec((BLK, dim), glob), pl.BlockSpec((BLK, LANE), glob),
                  pl.BlockSpec((1, dim, ffn), wmap), pl.BlockSpec((1, dim, ffn), wmap), pl.BlockSpec((1, ffn, dim), wmap)],
        out_specs=[pl.BlockSpec((BLK, dim), loc), pl.BlockSpec((BLK, dim), loc), pl.BlockSpec((BLK, LANE), loc)]
        + [pl.BlockSpec((BLK, ffn), glob)] * 3)(x, dy, g, w1, w3, w2, *outs)


def run_experts(x_rows, dy_rows, gates, w1, w3, w2, saved, blk_e, meta):
    n_rows, dim = x_rows.shape
    loc_rows = blk_e.shape[0] * BLK
    return pl.pallas_call(
        expert_kernel,
        out_shape=[jax.ShapeDtypeStruct((loc_rows, dim), BF16), jax.ShapeDtypeStruct((loc_rows, dim), BF16),
                   jax.ShapeDtypeStruct((loc_rows, LANE), F32)] + [jax.ShapeDtypeStruct((n_rows, w1.shape[2]), BF16)] * 3,
        in_specs=[SMEM] * 2 + [HBM] * (6 + len(saved)),
        out_specs=[HBM] * 6,
        input_output_aliases={8 + i: 3 + i for i in range(len(saved))},
        compiler_params=pltpu.CompilerParams(**PARAMS),
        cost_estimate=pl.CostEstimate(flops=55_000_000_000, bytes_accessed=120_000_000, transcendentals=0),
        name="experts",
    )(blk_e, meta, x_rows, dy_rows, gates, w1, w3, w2, *saved)


def combine_kernel(where, n_groups, slot_cap, blk_e, blk_k, blk_n, meta, slots, o_hbm, dx_hbm, g_hbm, dg_hbm, *refs):
    out_ref, dgo_ref, stage_y, stage_dx, stage_dg, buf_y, buf_dx, sem = refs[-8:]
    n_chip = out_ref.shape[0]
    lines = out_ref.shape[3]
    chunk_tok = n_chip * lines // n_groups
    dim = n_groups * LANE
    off = meta[1]

    def rows(b, o_ref, dx_ref, g_ref, dg_ref):
        base = blk_e[b] * slot_cap + blk_k[b] * BLK
        n_used = jnp.minimum(blk_n[b], BLK)

        def unpack(i, carry):
            g16 = g_ref[sixteen(i), :]
            for c in range(n_groups):
                lanes = slice(c * LANE, (c + 1) * LANE)
                rows_to_lines(buf_y, i * 16, o_ref[sixteen(i), lanes].astype(F32) * g16, c, n_groups)
                rows_to_lines(buf_dx, i * 16, dx_ref[sixteen(i), lanes].astype(F32), c, n_groups)
            return carry
        lax.fori_loop(0, pl.cdiv(n_used, 16), unpack, 0)

        def add(g, carry):
            todo = []
            for r in range(SUB):
                t = slots[base + g * SUB + r]
                new = []
                for stage, buf in ((stage_y, buf_y), (stage_dx, buf_dx)):
                    a, b2 = lines_of(buf, g * SUB + r, n_groups)
                    old_a, old_b = lines_of(stage, t, n_groups)
                    new.append((old_a + a, old_b + b2))
                todo.append((t, new, stage_dg[pl.ds(t, 1), :] + dg_ref[pl.ds(g * SUB + r, 1), :]))
            for t, new, more in todo:
                put_lines(stage_y, t, n_groups, new[0])
                put_lines(stage_dx, t, n_groups, new[1])
                stage_dg[pl.ds(t, 1), :] = more
            return carry
        lax.fori_loop(0, pl.cdiv(n_used, SUB), add, 0)

    clear_lines(stage_y, chunk_tok * n_groups)
    clear_lines(stage_dx, chunk_tok * n_groups)
    clear_lines(stage_dg, chunk_tok)
    loc = lambda i: (i, 0)
    pipeline(rows, meta[0], in_specs=[pl.BlockSpec((BLK, dim), loc), pl.BlockSpec((BLK, dim), loc), pl.BlockSpec((BLK, LANE), lambda i: (off + i, 0)),
                                      pl.BlockSpec((BLK, LANE), loc)])(o_hbm, dx_hbm, g_hbm, dg_hbm)
    copies = [pltpu.make_async_copy(stage.at[pl.ds(j * lines, lines)], out_ref.at[j, where, which], sem.at[which])
              for which, stage in enumerate((stage_y, stage_dx)) for j in range(n_chip)]
    copies.append(pltpu.make_async_copy(stage_dg.at[pl.ds(0, chunk_tok)], dgo_ref, sem.at[2]))
    for copy in copies:
        copy.start()
    for copy in copies:
        copy.wait()


def combine_rows(o_rows, gates, dg, dx_rows, tables, chunk_tok, n_chip, where, n_held, held):
    n_groups = o_rows.shape[1] // LANE
    blk_e, blk_k, blk_n, meta, slots, _, n_exp = tables
    more = [] if held is None else [held]
    stage = pltpu.VMEM(((chunk_tok + 2) * n_groups, LANE), F32)
    buf = pltpu.VMEM((BLK * n_groups, LANE), F32)
    return pl.pallas_call(
        functools.partial(combine_kernel, where, n_groups, slots.shape[0] // n_exp),
        out_shape=[jax.ShapeDtypeStruct((n_chip, n_held, 2, chunk_tok * n_groups // n_chip, LANE), F32), jax.ShapeDtypeStruct((chunk_tok, LANE), F32)],
        in_specs=[SMEM] * 5 + [HBM] * (4 + len(more)),
        out_specs=[HBM] * 2,
        input_output_aliases={} if held is None else {9: 0},
        scratch_shapes=[stage, stage, pltpu.VMEM((chunk_tok + SUB, LANE), F32), buf, buf, pltpu.SemaphoreType.DMA((3,))],
        compiler_params=pltpu.CompilerParams(**PARAMS),
        cost_estimate=pl.CostEstimate(flops=30_000_000_000, bytes_accessed=120_000_000, transcendentals=0),
        name="combine_rows",
    )(blk_e, blk_k, blk_n, meta, slots, o_rows, dx_rows, gates, dg, *more)


def grad_kernel(first_expert, last_out, order, owner, span, *refs):
    n_in = 6 if last_out else 9
    ins, outs, accs = refs[:n_in], refs[n_in:n_in + 3], refs[n_in + 3:]
    dim, ffn = outs[0].shape[1:]
    start, n = span[0], span[1]

    def step(i, x_ref, dy_ref, g_ref, h_ref, d1_ref, d3_ref, *rest):
        at = start + i
        e = owner[at]
        first = jnp.logical_or(i == 0, owner[jnp.maximum(at - 1, 0)] != e)
        last = jnp.logical_or(i == n - 1, owner[jnp.minimum(at + 1, owner.shape[0] - 1)] != e)

        @pl.when(first)
        def _():
            for acc in accs:
                acc[...] = jnp.zeros_like(acc)

        x = x_ref[...]
        accs[0][...] += dot_lt(x, d1_ref[...])
        accs[1][...] += dot_lt(x, d3_ref[...])
        accs[2][...] += dot_lt(h_ref[...], scale_rows(g_ref[...], dy_ref[...].astype(F32)))

        @pl.when(last)
        def _():
            for k, acc in enumerate(accs):
                if last_out:
                    rest[k][0] = acc[...]
                else:
                    rest[3 + k][0] = (acc[...] + rest[k][0]).astype(BF16)
    row = lambda i: (order[start + i], 0)
    wmap = lambda i: (owner[start + i] - first_expert, 0, 0)
    up, down = pl.BlockSpec((1, dim, ffn), wmap), pl.BlockSpec((1, ffn, dim), wmap)
    pipeline(
        step, n,
        in_specs=[pl.BlockSpec((BLK, dim), row), pl.BlockSpec((BLK, dim), row), pl.BlockSpec((BLK, LANE), row)]
        + [pl.BlockSpec((BLK, ffn), row)] * 3 + ([] if last_out else [up, up, down]),
        out_specs=[up, up, down],
    )(*ins, *outs)


def weight_grads(x_rows, dy_rows, gates, saved, order, owner, span, n_local, first_expert, theirs):
    dim = x_rows.shape[1]
    ffn = saved[0].shape[1]
    out = BF16 if theirs else F32
    return pl.pallas_call(
        functools.partial(grad_kernel, first_expert, not theirs),
        out_shape=[jax.ShapeDtypeStruct((n_local, dim, ffn), out), jax.ShapeDtypeStruct((n_local, dim, ffn), out),
                   jax.ShapeDtypeStruct((n_local, ffn, dim), out)],
        in_specs=[SMEM] * 3 + [HBM] * (6 + len(theirs)),
        out_specs=[HBM] * 3,
        scratch_shapes=[pltpu.VMEM((dim, ffn), F32), pltpu.VMEM((dim, ffn), F32), pltpu.VMEM((ffn, dim), F32)],
        compiler_params=pltpu.CompilerParams(**PARAMS),
        cost_estimate=pl.CostEstimate(flops=55_000_000_000, bytes_accessed=160_000_000, transcendentals=0),
        name="grads_own" if theirs else "grads_other",
    )(order, owner, span, x_rows, dy_rows, gates, *saved, *theirs)


def shared_kernel(n_arr, n_dev, place, *refs):
    toks = refs[:n_arr]
    w1_ref, w3_ref, w2_ref, o1_ref, o3_ref, o2_ref, own_ref, xbuf, dybuf, hbuf, d1buf, d3buf, outbuf, sem, out_sem = refs[n_arr:]
    chip = place[0]
    per_half = n_arr * PER_GATHER * n_dev
    total = 2 * per_half

    def copies(k, dev, chunk, slot):
        row = dev * 2 * PER_GATHER + chunk
        return (pltpu.make_async_copy(toks[k].at[pl.ds(row * STAGE, STAGE)], xbuf.at[slot], sem.at[slot, 0]),
                pltpu.make_async_copy(toks[k].at[pl.ds((row + PER_GATHER) * STAGE, STAGE)], dybuf.at[slot], sem.at[slot, 1]))

    def place_of(i):
        j = lax.rem(i, per_half)
        which = j // n_dev
        return which, j - which * n_dev

    def fetch(i, slot):
        which, dev = place_of(i)
        for k in range(n_arr):
            @pl.when(which // PER_GATHER == k)
            def _():
                for copy in copies(k, dev, which - k * PER_GATHER, slot):
                    copy.start()

    fetch(0, 0)
    for ref in (o1_ref, o3_ref, o2_ref):
        ref[...] = jnp.zeros_like(ref)

    def step(i, carry):
        slot = lax.rem(i, 2)
        half = i // per_half
        which, dev = place_of(i)

        @pl.when(i + 1 < total)
        def _():
            fetch(i + 1, 1 - slot)
        for copy in copies(0, 0, 0, slot):
            copy.wait()
        x = xbuf[slot]
        dy = dybuf[slot]
        b1 = dot(x, w1_ref[half])
        b3 = dot(x, w3_ref[half])
        sig = jax.nn.sigmoid(b1)
        act = b1 * sig
        h = (act * b3).astype(BF16)
        hbuf[...] = h
        o2_ref[half] += dot_lt(h, dy)
        dh = dot_rt(dy, w2_ref[half])
        d1 = (dh * b3 * (sig * (1.0 + b1 * (1.0 - sig)))).astype(BF16)
        d1buf[...] = d1
        o1_ref[half] += dot_lt(x, d1)
        d3 = (dh * act).astype(BF16)
        d3buf[...] = d3
        o3_ref[half] += dot_lt(x, d3)

        @pl.when(dev == chip)
        def _():
            outbuf[0] = dot(hbuf[...], w2_ref[half])
            outbuf[1] = dot_rt(d1buf[...], w1_ref[half]) + dot_rt(d3buf[...], w3_ref[half])
            put = pltpu.make_async_copy(outbuf, own_ref.at[half, :, pl.ds(which * STAGE, STAGE)], out_sem)
            put.start()
            put.wait()
        return carry
    lax.fori_loop(0, total, step, 0)


def shared_expert(toks, w1, w3, w2, chip, n_dev):
    _, dim, width = w1.shape
    small = pltpu.VMEM((STAGE, width), BF16)
    return pl.pallas_call(
        functools.partial(shared_kernel, len(toks), n_dev),
        out_shape=[jax.ShapeDtypeStruct((2, dim, width), F32), jax.ShapeDtypeStruct((2, dim, width), F32), jax.ShapeDtypeStruct((2, width, dim), F32),
                   jax.ShapeDtypeStruct((2, 2, CHUNKS * STAGE, dim), F32)],
        in_specs=[SMEM] + [HBM] * len(toks) + [VMEM] * 3,
        out_specs=[VMEM] * 3 + [HBM],
        scratch_shapes=[pltpu.VMEM((2, STAGE, dim), BF16), pltpu.VMEM((2, STAGE, dim), BF16), small, small, small,
                        pltpu.VMEM((2, STAGE, dim), F32), pltpu.SemaphoreType.DMA((2, 2)), pltpu.SemaphoreType.DMA],
        compiler_params=pltpu.CompilerParams(**PARAMS),
        cost_estimate=pl.CostEstimate(flops=170_000_000_000, bytes_accessed=160_000_000, transcendentals=0),
        name="shared_expert",
    )(chip[None], *toks, w1, w3, w2)


def finish_kernel(n_groups, sum_ref, own_ref, *refs):
    y_ref, dx_ref = refs[-2:]

    def body(i, carry):
        for which, out in ((0, y_ref), (1, dx_ref)):
            for c in range(n_groups):
                lanes = slice(c * LANE, (c + 1) * LANE)
                val = lines_to_rows(sum_ref.at[0, 0, which], i * 16, c, n_groups) + (own_ref[0, which, sixteen(i), lanes] + own_ref[1, which, sixteen(i), lanes])
                out[sixteen(i), lanes] = val.astype(BF16)
        return carry
    lax.fori_loop(0, y_ref.shape[0] // 16, body, 0)


def finish(chunk, sums, where, own, held):
    n_tok, dim = own.shape[2:]
    n_groups = dim // LANE
    part = STAGE // 2
    row = pl.BlockSpec((part, dim), lambda i: (2 * chunk + i, 0))
    return pl.pallas_call(
        functools.partial(finish_kernel, n_groups),
        out_shape=[jax.ShapeDtypeStruct((n_tok, dim), BF16)] * 2,
        grid=(2,),
        in_specs=[pl.BlockSpec((1, 1, 2, part * n_groups, LANE), lambda i: (0, where, 0, i, 0)),
                  pl.BlockSpec((2, 2, part, dim), lambda i: (0, 0, 2 * chunk + i, 0))] + [HBM] * len(held),
        out_specs=[row, row],
        input_output_aliases={2 + i: i for i in range(len(held))},
        compiler_params=pltpu.CompilerParams(dimension_semantics=("arbitrary",), **PARAMS),
        cost_estimate=pl.CostEstimate(flops=4_000_000_000, bytes_accessed=20_000_000, transcendentals=0),
        name="finish",
    )(sums, own, *held)


def route(ids_all, gates_all, experts, slot_cap):
    n_chunk, n_top, chunk_tok = ids_all.shape
    n_exp = experts.shape[0]
    match = ids_all[:, None] == experts[None, :, None, None]
    hit = jnp.any(match, axis=2)
    gsel = jnp.sum(jnp.where(match, gates_all[:, None], 0.0), axis=2)
    n_seg = chunk_tok // LANE
    strict = (jnp.arange(LANE)[:, None] < jnp.arange(LANE)[None, :]).astype(BF16)
    seg = hit.reshape(n_chunk, n_exp, n_seg, LANE)
    inner = jnp.einsum('cesl,lm->cesm', seg.astype(BF16), strict, preferred_element_type=F32)
    seg_sum = jnp.sum(seg, axis=3, dtype=jnp.int32)
    before = jnp.arange(n_seg)[:, None] < jnp.arange(n_seg)[None, :]
    outer = jnp.sum(jnp.where(before, seg_sum[..., :, None], 0), axis=2)
    rank = (inner.astype(jnp.int32) + outer[..., None]).reshape(n_chunk, n_exp, chunk_tok)
    count = jnp.sum(seg_sum, axis=2)
    n_hi = slot_cap // 64
    hi = jnp.where(hit, rank >> 6, -1)
    lo = rank & 63
    pick_hi = (hi[:, :, None, :] == jnp.arange(n_hi, dtype=jnp.int32)[:, None]).astype(BF16)
    tok = jnp.arange(chunk_tok, dtype=jnp.int32)
    pick_lo = lo[:, :, None, :] == jnp.arange(64, dtype=jnp.int32)[:, None]
    val_lo = jnp.concatenate([jnp.where(pick_lo, (tok >> 6), 0), jnp.where(pick_lo, (tok & 63), 0)], axis=2).astype(BF16)
    found = jnp.einsum('ceht,cent->cehn', pick_hi, val_lo, preferred_element_type=F32).astype(jnp.int32)
    slots = (found[..., :64] * 64 + found[..., 64:]).reshape(n_chunk, n_exp, slot_cap)
    slots = jnp.where(jnp.arange(slot_cap, dtype=jnp.int32) < count[..., None], slots, chunk_tok)
    n_blk = (count + BLK - 1) // BLK
    upto = jnp.cumsum(n_blk, axis=1)
    chunk_blk = upto[:, -1]
    chunk_off = jnp.cumsum(chunk_blk) - chunk_blk
    max_blk = n_exp * (slot_cap // BLK)
    at = jnp.arange(max_blk, dtype=jnp.int32)
    blk_e = jnp.minimum(jnp.sum(at[None, :, None] >= upto[:, None, :], axis=2, dtype=jnp.int32), n_exp - 1)
    start = upto - n_blk
    of_blk = lambda v: jnp.sum(jnp.where(blk_e[..., None] == jnp.arange(n_exp), v[:, None, :], 0), axis=2, dtype=jnp.int32)
    blk_k = at[None, :] - of_blk(start)
    blk_n = jnp.maximum(of_blk(count) - blk_k * BLK, 0)
    glob = (chunk_off[:, None] + start).T.reshape(-1)
    cnt = n_blk.T.reshape(-1)
    end = jnp.cumsum(cnt)
    own_blk = end[n_exp // 2 * n_chunk - 1]
    at2 = jnp.arange(max_blk + n_chunk * n_exp, dtype=jnp.int32)
    grp = jnp.minimum(jnp.sum(at2[:, None] >= end[None, :], axis=1, dtype=jnp.int32), cnt.shape[0] - 1)
    sel = grp[:, None] == jnp.arange(cnt.shape[0])
    order = at2 + jnp.sum(jnp.where(sel, (glob - (end - cnt))[None, :], 0), axis=1)
    order = jnp.clip(order, 0, at2.shape[0] - 1).astype(jnp.int32)
    owner = (grp // n_chunk).astype(jnp.int32)
    spans = jnp.stack([jnp.stack([jnp.zeros_like(own_blk), own_blk]), jnp.stack([own_blk, end[-1] - own_blk])]).astype(jnp.int32)
    return slots, gsel, jnp.stack([blk_e, blk_k, blk_n]).astype(jnp.int32), chunk_blk, chunk_off, order, owner, spans


def solution(mesh):
    ei_size = mesh.shape['ei']
    ex_size = mesh.shape['eo'] // 2
    n_chip = ei_size * ex_size
    group_size = 2 * n_chip
    split_mesh = jax.sharding.Mesh(mesh.devices.reshape(mesh.shape['dp'], ei_size, ex_size, 2), ('dp', 'ei', 'ex', 'core'))
    axes = ('ei', 'ex', 'core')
    chips = ('ei', 'ex')
    tok_spec = P(('dp', *axes), None)
    exp_spec = P(axes, None, None)
    full_spec = P(None, None)
    grad_spec = P(('dp', *axes), None, None)
    shared_spec = P('dp', None)

    def swap(v):
        return lax.ppermute(v, 'core', [(0, 1), (1, 0)])

    def device_step(x_loc, ids_loc, gates_loc, w_one, w_three, w_two, s_one, s_three, s_two, dy_loc):
        n_tok, n_top = ids_loc.shape
        dim = x_loc.shape[1]
        n_local = w_one.shape[0]
        n_exp = n_local * group_size
        n_here = 2 * n_local
        cap = min(n_tok, CAP_FACTOR * ((n_tok * n_top + n_exp - 1) // n_exp))
        slot_cap = cap * n_chip
        part = n_tok // CHUNKS
        chunk_tok = part * n_chip
        core = lax.axis_index('core')
        chip = lax.axis_index('ei') * ex_size + lax.axis_index('ex')

        span = PER_GATHER * part
        mine = [jnp.concatenate([v[k * span:(k + 1) * span] for v in (x_loc, dy_loc)]) for k in range(CHUNKS // PER_GATHER)]
        toks = [lax.all_gather(v, chips, axis=0, tiled=True) for v in lax.optimization_barrier(mine)]

        weights = [jnp.concatenate([w, swap(w)]) for w in (w_one, w_three, w_two)]
        near = (2 * chip + core) * n_local + jnp.arange(n_local, dtype=jnp.int32)
        far = (2 * chip + 1 - core) * n_local + jnp.arange(n_local, dtype=jnp.int32)

        both = lax.all_gather(jnp.concatenate([ids_loc.T.astype(F32), gates_loc.T]), chips, axis=0)
        both = both.reshape(n_chip, 2 * n_top, CHUNKS, part).transpose(2, 1, 0, 3).reshape(CHUNKS, 2 * n_top, chunk_tok)
        slots, gsel, blks, chunk_blk, chunk_off, order, owner, spans = route(
            both[:, :n_top].astype(jnp.int32), both[:, n_top:], jnp.concatenate([near, far]), slot_cap)
        n_rows = order.shape[0] * BLK

        held, saved = [], []
        sums, dg_parts = {}, []
        for c in range(CHUNKS):
            meta = jnp.stack([chunk_blk[c], chunk_off[c]]).astype(jnp.int32)
            gpad = jnp.concatenate([gsel[c].reshape(-1), jnp.zeros((LANE,), F32)])
            tables = (*blks[:, c], meta, slots[c].reshape(-1), gpad, n_here)
            x_rows, dy_rows, gate_rows = gather_rows(c % PER_GATHER, toks[c // PER_GATHER], held, tables, n_rows, n_chip)
            o_rows, dx_rows, dg, *saved = run_experts(x_rows, dy_rows, gate_rows, *weights, saved, tables[0], meta)
            (group,) = [g for g in SCATTERS if c in g]
            where = group.index(c)
            total, dg_part = combine_rows(o_rows, gate_rows, dg, dx_rows, tables, chunk_tok, n_chip, where, len(group), sums[c - 1] if where else None)
            x_rows, total = lax.optimization_barrier((x_rows, total))
            held = [x_rows, dy_rows, gate_rows]
            sums[c] = total
            if c == group[-1]:
                total = lax.psum_scatter(total, chips, scatter_dimension=0, tiled=True)
                for k in group:
                    sums[k] = total
            dg_parts.append(dg_part[:, :n_here].T.reshape(n_here, n_chip, part))

        rows = (x_rows, dy_rows, gate_rows, saved, order, owner)
        others = weight_grads(*rows, spans[1], n_local, n_local, [])
        theirs = [swap(v) for v in others]
        width = s_one.shape[1] // 2
        toks, theirs_ = lax.optimization_barrier((toks, others[0]))
        cut = lambda w: jnp.stack([w[:, :width], w[:, width:]])
        *shared, own = shared_expert(toks, cut(s_one), cut(s_three), s_two.reshape(2, width, dim), chip, n_chip)
        theirs, own = lax.optimization_barrier((theirs, own))
        dw_one, dw_three, dw_two = weight_grads(*rows, spans[0], n_local, 0, theirs)

        pair = lambda v: v + swap(v)
        dws_one, dws_three = (jnp.concatenate([v[0], v[1]], axis=1) for v in (pair(shared[0]), pair(shared[1])))
        dws_two = pair(shared[2]).reshape(2 * width, dim)

        dg_send = jnp.concatenate(dg_parts, axis=2).transpose(1, 0, 2)
        dg_recv = lax.all_to_all(dg_send, chips, 0, 0).reshape(n_chip, 2, n_local, n_tok)
        dg_tok = jnp.where(core == 0, dg_recv, jnp.flip(dg_recv, 1)).reshape(n_exp, n_tok)
        pick = ids_loc.T[:, None, :] == jnp.arange(n_exp, dtype=jnp.int32)[:, None]
        d_gates = jnp.sum(jnp.where(pick, dg_tok[None], 0.0), axis=1).T

        outs = []
        for c in range(CHUNKS):
            outs = finish(c, sums[c], sum(g.index(c) for g in SCATTERS if c in g), own, outs)
        y_loc, dx_loc = outs
        return (y_loc, dx_loc, d_gates, dw_one, dw_three, dw_two, dws_one, dws_three, dws_two)

    return jax.shard_map(device_step, mesh=split_mesh, in_specs=(tok_spec, tok_spec, tok_spec, exp_spec, exp_spec, exp_spec, full_spec, full_spec, full_spec, tok_spec), out_specs=(tok_spec, tok_spec, tok_spec, grad_spec, grad_spec, grad_spec, shared_spec, shared_spec, shared_spec), check_vma=False)
```
